256 devices in a mesh: row: 8 (over z), col: 16 (over y_lo, x, core), layer: 2 (over y_hi).
Axes of the slice: x: 4, y: 4 (y_hi: 2, y_lo: 2; y = y_hi * 2 + y_lo), z: 8, core: 2. Of those that a mesh axis runs over, the one named last changes fastest.
Arguments:
- left: bfloat16 [8192, 8192], P('row', ('col', 'layer')), may hold values from -6 to 6
- middle: bfloat16 [8192, 8192], P('row', 'col'), may hold values from -0.0625 to 0.0625
- right: bfloat16 [8192, 8192], P('row', 'col'), may hold values from -0.0625 to 0.0625
Outputs:
- product: bfloat16 [8192, 8192], P('row', ('col', 'layer'))
The draws below stay inside these ranges and needn't reach their ends.
All inputs are finite; a program needn't handle non-finite values.
Results may differ from the reference program's by a relative error of at most 0.0049.
Values may be sent and summed in bfloat16 or wider, within the bound.
A program may use at most 64 MiB of HBM per device.

```python
import jax
import jax.numpy as jnp

K = 8192
N = 8192
P_SIZE = 8192
M = 8192


def block_scale(rng, dims, pieces, low, high):
    loudness, own = 1.0, jax.random.fold_in(rng, 6)
    for axis_at, shards_of in pieces:
        heights = jnp.exp(jax.random.uniform(jax.random.fold_in(own, axis_at), (shards_of,), jnp.float32, low / len(pieces), high / len(pieces)))
        loudness = loudness * jnp.repeat(heights, dims[axis_at] // shards_of).reshape([-1 if axis == axis_at else 1 for axis in range(len(dims))])
    return loudness


def scatter_about(key, dims, deviation, limit, shards=(), kind=jnp.bfloat16):
    array = jax.random.normal(key, dims, jnp.float32) * deviation
    if len(shards) > 0:
        array = block_scale(key, dims, shards, -0.22, 0.18) * array
    return jnp.clip(array, min=-limit, max=limit).astype(kind)


def setup_inputs(seed: int = 0) -> dict:
    streams_of = jax.random.split(jax.random.key(seed), 4)
    return {
        "left": scatter_about(streams_of[0], (M, K), 1.0, 6.0, ((0, 8), (1, 32))),
        "middle": scatter_about(streams_of[1], (K, N), K ** -0.5, 0.0625, ((0, 8), (1, 16))),
        "right": scatter_about(streams_of[2], (N, P_SIZE), N ** -0.5, 0.0625, ((0, 8), (1, 16))),
    }


def reference(left, middle, right):
    first = jnp.dot(left, middle, preferred_element_type=jnp.float32).astype(jnp.bfloat16)
    return jnp.dot(first, right, preferred_element_type=jnp.float32).astype(jnp.bfloat16)
```

```python
import jax
import jax.numpy as jnp
from jax import lax
from jax.experimental import pallas as pl
from jax.experimental.pallas import tpu as pltpu
from jax.sharding import PartitionSpec as P

MESH = pl.DeviceIdType.MESH
BF16 = jnp.bfloat16
TM = 256
TILES = 1024 // TM

STAGES = [(0, 0), (0, 1), (0, 2), (0, 3), (1, 0), (1, 1), (1, 2), (1, 3)]

ORDER = [
    (1, 0), (0, 0), (1, 1), (0, 1), (1, 2), (0, 2), (1, 3), (0, 3),
    (2, 0), (3, 0), (2, 1), (3, 1), (2, 2), (3, 2), (2, 3), (4, 0), (3, 3),
    (5, 0), (4, 1), (5, 1), (4, 2), (6, 0), (4, 3), (5, 2), (6, 1), (5, 3), (7, 0),
    (6, 2), (7, 1), (6, 3), (7, 2), (7, 3),
]


def rem(a, n):
    return lax.rem(a + 4 * n, jnp.int32(n))


def kernel(left, middle, right, out, A, B, send, recv, obuf,
           bar_unused, zS, zR, xS, xR, dS, dR, cS, cR, hS, hR, wS, wR, lS, oS):
    z = lax.axis_index("row")
    col = lax.axis_index("col")
    h = lax.axis_index("layer")
    c = lax.rem(col, 2)
    x = lax.rem(lax.div(col, 2), 4)
    lo = lax.div(col, 8)
    y = h * 2 + lo

    def dev(zz=None, xx=None, yy=None, cc=None):
        zz = z if zz is None else zz
        xx = x if xx is None else xx
        yy = y if yy is None else yy
        cc = c if cc is None else cc
        return (zz, lax.rem(yy, 2) * 8 + xx * 2 + cc, lax.div(yy, 2))

    z_to = [dev(zz=rem(z + 1, 8)), dev(zz=rem(z - 1, 8))]
    x_to = [dev(xx=rem(x + 1, 4)), dev(xx=rem(x - 1, 4))]
    y_of = [dev(yy=rem(y + d, 4)) for d in (1, 2, 3)]
    pair = dev(yy=h * 2 + 1 - lo)
    yt = h * 2 + 1 - lo
    core = dev(cc=1 - c)

    barrier = pltpu.get_barrier_semaphore()
    for peer in z_to + x_to + y_of + [core]:
        pl.semaphore_signal(barrier, inc=1, device_id=peer, device_id_type=MESH)

    def m128(v):
        return pl.multiple_of(v, 128)

    def zpos(zz):
        return lax.rem(zz, 4) * 2 + lax.div(zz, 4)

    def local(src, dst, sem):
        return pltpu.make_async_copy(src, dst, sem)

    def remote(src, dst, ssem, rsem, to):
        return pltpu.make_async_remote_copy(
            src_ref=src, dst_ref=dst, send_sem=ssem, recv_sem=rsem, device_id=to, device_id_type=MESH
        )

    ymod = lambda v: rem(v, 4)

    def own_rows(p, j, cols_from, width, cols_to, ywho):
        src = (middle, right)[p].at[:, pl.ds(m128(ywho * 128), 128), pl.ds(m128(cols_from), width)]
        dst = B.at[p, j, :, zpos(z), :, pl.ds(cols_to, width)]
        return src, dst

    def own_parts(yw, l_src):
        own = [
            (0, 1, ymod(yw + 1) * 128, 128, 0),
            (0, 1, ymod(yw + 3) * 128, 128, 128),
            (0, 0, ymod(yw + 2) * 128, 128, m128(l_src * 128)),
            (0, 3, yw * 128, 128, m128(l_src * 128)),
            (1, 0, lax.div(ymod(yw + 2), 2) * 256, 256, 0),
            (1, 3, lax.div(yw, 2) * 256, 256, 0),
        ]
        hop = [
            (0, 0, ymod(yw + 2) * 128, 128, m128(l_src * 128)),
            (0, 2, ymod(yw + 1) * 128, 128, 0),
            (0, 2, ymod(yw + 3) * 128, 128, 128),
            (0, 3, yw * 128, 128, m128(l_src * 128)),
            (1, 1, lax.div(ymod(yw + 1), 2) * 256, 128, 0),
            (1, 1, lax.div(ymod(yw + 3), 2) * 256, 128, 128),
            (1, 2, lax.div(ymod(yw + 1), 2) * 256 + 128, 128, 0),
            (1, 2, lax.div(ymod(yw + 3), 2) * 256 + 128, 128, 128),
        ]
        return own, hop

    own, _ = own_parts(y, lo)
    _, hop_out = own_parts(yt, lo)
    _, hop_in = own_parts(y, 1 - lo)
    own_copies = [local(*own_rows(p, j, f, w, t, y), lS.at[i]) for i, (p, j, f, w, t) in enumerate(own)]
    hop_sends = [
        remote(*own_rows(p, j, f, w, t, yt), hS.at[i], hR.at[i], pair) for i, (p, j, f, w, t) in enumerate(hop_out)
    ]
    hop_recvs = [
        remote(*own_rows(p, j, f, w, t, y), hS.at[i], hR.at[i], pair) for i, (p, j, f, w, t) in enumerate(hop_in)
    ]

    def strip(cc, xx):
        return (cc * 4 + xx) * 256

    def xregion(p, cc, xx, u):
        if p == 0:
            half = lo if u < 2 else 1 - lo
            return A.at[0, pl.ds((u % 2) * 512, 512), pl.ds(m128(strip(cc, xx) + half * 128), 128)]
        return A.at[1, pl.ds(u * TM, TM), pl.ds(m128(strip(cc, xx)), 256)]

    left_copy = local(
        left.at[:, pl.ds(m128(lo * 128), 128)],
        A.at[0, :, pl.ds(m128(strip(c, x) + lo * 128), 128)],
        lS.at[6],
    )
    swaps = [
        remote(
            left.at[pl.ds(u * 512, 512), pl.ds(m128((1 - lo) * 128), 128)],
            A.at[0, pl.ds(u * 512, 512), pl.ds(m128(strip(c, x) + lo * 128), 128)],
            wS.at[u], wR.at[u], pair,
        )
        for u in range(2)
    ]
    swap_recvs = [
        remote(
            left.at[pl.ds(u * 512, 512), pl.ds(m128((1 - lo) * 128), 128)],
            A.at[0, pl.ds(u * 512, 512), pl.ds(m128(strip(c, x) + (1 - lo) * 128), 128)],
            wS.at[u], wR.at[u], pair,
        )
        for u in range(2)
    ]

    left_copy.start()
    for i in range(6):
        own_copies[i].start()

    pl.semaphore_wait(barrier, 8)

    sent = []

    def go(copy):
        copy.start()
        sent.append(copy)

    go(hop_sends[0])
    for u in range(2):
        go(swaps[u])
    for i in range(1, 8):
        go(hop_sends[i])

    OWN_OF = {(0, 0): [2], (0, 1): [0, 1], (0, 2): [], (0, 3): [3], (1, 0): [4], (1, 1): [], (1, 2): [], (1, 3): [5]}
    HOP_OF = {(0, 0): [0], (0, 1): [], (0, 2): [1, 2], (0, 3): [3], (1, 0): [], (1, 1): [4, 5], (1, 2): [6, 7], (1, 3): []}

    def z_copy(s, d, minor, level, arriving):
        p, j = STAGES[s]
        sign = -1 if d == 0 else 1
        half = d if minor == 0 else 1 - d
        block = rem(z + sign * (level + (1 if arriving else 0)), 8)
        ref = B.at[p, j, half, zpos(block)]
        k = level + (4 if minor else 0)
        return remote(ref, ref, zS.at[d, s, k], zR.at[d, s, k], z_to[d])

    def z_tick(s, level):
        if level == 0:
            for i in OWN_OF[STAGES[s]]:
                own_copies[i].wait()
            for i in HOP_OF[STAGES[s]]:
                hop_recvs[i].wait_recv()
        for minor in range(2):
            if minor == 1 and level == 3:
                continue
            for d in range(2):
                if level > 0:
                    z_copy(s, d, minor, level - 1, True).wait_recv()
                go(z_copy(s, d, minor, level, False))

    def z_last(s):
        for d in range(2):
            z_copy(s, d, 1, 2, True).wait_recv()
            z_copy(s, d, 0, 3, True).wait_recv()

    def x_copy(p, d, u, forward, arriving):
        sign = -1 if d == 0 else 1
        away = (1 if forward else 0) + (1 if arriving else 0)
        ref = xregion(p, c, rem(x + sign * away, 4), u)
        k = 4 + u // 2 if forward else u
        return remote(ref, ref, xS.at[p, d, k], xR.at[p, d, k], x_to[d])

    def x_forward(p, d, u):
        x_copy(p, d, u, False, True).wait_recv()
        go(x_copy(p, d, u, True, False))

    def d_copy(p, away, u, arriving):
        cc = 1 - c if arriving else c
        ref = xregion(p, cc, rem(x + away, 4), u)
        return remote(ref, ref, dS.at[p, away, u], dR.at[p, away, u], core)

    def d_all(p):
        for away in range(4):
            for u in range(4):
                d_copy(p, away, u, True).wait_recv()

    def c_copies(p, j, t, arriving):
        rows = pl.ds(t * TM, TM)
        if j == 0:
            return [remote(send.at[p, 0, rows], recv.at[p, 1, rows], cS.at[p, 0, t], cR.at[p, 0, t], y_of[1])]
        made = []
        for q in range(2):
            if p == 0:
                which = lo if (j == 1) != arriving else 1 - lo
                place = m128(which * 128)
            else:
                place = (j - 1) * 128
            k = 1 + (j - 1) * 2 + q
            made.append(
                remote(
                    send.at[p, j, rows, pl.ds(q * 128, 128)],
                    recv.at[p, 2 * q, rows, pl.ds(place, 128)],
                    cS.at[p, k, t], cR.at[p, k, t], y_of[2 * q],
                )
            )
        return made

    def compute(s, t0, t1):
        p, j = STAGES[s]

        def body(t, carry):
            rows = pl.ds(pl.multiple_of(t * TM, TM), TM)
            acc = jnp.dot(A[p, rows, :], B[p, j].reshape(2048, 256), preferred_element_type=jnp.float32)
            if j < 3:
                send[p, j, rows, :] = acc.astype(BF16)
                for copy in c_copies(p, j, t, False):
                    copy.start()
                return carry
            for jj in range(3):
                for copy in c_copies(p, jj, t, True):
                    copy.wait_recv()
            for d in range(3):
                acc = acc + recv[p, d, rows, :].astype(jnp.float32)
            if p == 0:
                A[1, rows, pl.ds(m128(strip(c, x)), 256)] = acc.astype(BF16)
                own_strip = A.at[1, rows, pl.ds(m128(strip(c, x)), 256)]
                for d in range(2):
                    remote(own_strip, own_strip, xS.at[1, d, t], xR.at[1, d, t], x_to[d]).start()
                remote(own_strip, own_strip, dS.at[1, 0, t], dR.at[1, 0, t], core).start()
            else:
                obuf[rows, :] = acc.astype(BF16)
                local(obuf.at[rows], out.at[rows], oS.at[t]).start()
            return carry

        lax.fori_loop(t0, t1, body, 0)

    def x_start_own():
        left_copy.wait()
        for u in (0, 1):
            go(x_copy(0, 0, u, False, False))
            go(x_copy(0, 1, 1 - u, False, False))
            go(d_copy(0, 0, u, False))

    def x_start_swapped():
        for u in (2, 3):
            swap_recvs[u - 2].wait_recv()
        for u in (2, 3):
            go(x_copy(0, 0, u, False, False))
            go(x_copy(0, 1, 5 - u, False, False))
            go(d_copy(0, 0, u, False))

    def x_forwards(p, us):
        for u in us:
            d = u % 2
            x_forward(p, d, u)
            go(d_copy(p, 3 if d == 0 else 1, u, False))

    def x_rest(p, us):
        for u in us:
            d = 1 - u % 2
            x_copy(p, d, u, False, True).wait_recv()
            go(d_copy(p, 3 if d == 0 else 1, u, False))

    def x_far(p, us):
        for u in us:
            x_copy(p, u % 2, u, True, True).wait_recv()
            go(d_copy(p, 2, u, False))

    ACTIONS = {
        0: [x_start_own],
        3: [lambda: x_forwards(0, (0, 1))],
        4: [x_start_swapped, lambda: x_rest(0, (0, 1))],
        6: [lambda: x_forwards(0, (2, 3)), lambda: x_far(0, (0, 1))],
        7: [lambda: x_rest(0, (2, 3))],
        8: [lambda: z_last(1), lambda: z_last(0), lambda: x_far(0, (2, 3))],
        9: [lambda: d_all(0), lambda: compute(0, 0, 2)],
        10: [lambda: compute(0, 2, 4)],
        11: [lambda: compute(1, 0, 2)],
        12: [lambda: compute(1, 2, 4)],
        15: [lambda: z_last(2), lambda: compute(2, 0, 4)],
        17: [lambda: z_last(3), lambda: compute(3, 0, 4)],
        19: [lambda: x_forwards(1, (0, 1))],
        21: [lambda: x_forwards(1, (2, 3)), lambda: x_rest(1, (0, 1))],
        22: [lambda: x_rest(1, (2, 3))],
        23: [lambda: x_far(1, (0, 1))],
        24: [lambda: x_far(1, (2, 3)), lambda: z_last(4), lambda: d_all(1), lambda: compute(4, 0, 2)],
        25: [lambda: compute(4, 2, 4)],
        26: [lambda: z_last(5), lambda: compute(5, 0, 2)],
        27: [lambda: compute(5, 2, 4)],
        30: [lambda: z_last(6), lambda: compute(6, 0, 4)],
        31: [lambda: z_last(7), lambda: compute(7, 0, 4)],
    }
    for i, (s, level) in enumerate(ORDER):
        z_tick(s, level)
        for action in ACTIONS.get(i, ()):
            action()

    for copy in sent:
        copy.wait_send()
    for p in range(2):
        for j in range(3):
            for t in range(TILES):
                for copy in c_copies(p, j, t, False):
                    copy.wait_send()
    for t in range(TILES):
        for d in range(2):
            x_copy(1, d, t, False, False).wait_send()
        d_copy(1, 0, t, False).wait_send()
        local(obuf.at[pl.ds(t * TM, TM)], out.at[pl.ds(t * TM, TM)], oS.at[t]).wait()


def per_device(left, middle, right):
    rows, width = left.shape
    dma = pltpu.SemaphoreType.DMA
    return pl.pallas_call(
        kernel,
        out_shape=jax.ShapeDtypeStruct((rows, width), BF16),
        in_specs=[pl.BlockSpec(memory_space=pl.ANY)] * 3,
        out_specs=pl.BlockSpec(memory_space=pl.ANY),
        scratch_shapes=[
            pltpu.VMEM((2, 1024, 2048), BF16),
            pltpu.VMEM((2, 4, 2, 8, 128, 256), BF16),
            pltpu.VMEM((2, 3, 1024, 256), BF16),
            pltpu.VMEM((2, 3, 1024, 256), BF16),
            pltpu.VMEM((1024, 256), BF16),
            pltpu.SemaphoreType.REGULAR,
            dma((2, 8, 7)), dma((2, 8, 7)),
            dma((2, 2, 6)), dma((2, 2, 6)),
            dma((2, 4, 4)), dma((2, 4, 4)),
            dma((2, 5, TILES)), dma((2, 5, TILES)),
            dma((8,)), dma((8,)),
            dma((2,)), dma((2,)),
            dma((7,)),
            dma((TILES,)),
        ],
        compiler_params=pltpu.CompilerParams(
            collective_id=0, has_side_effects=True, vmem_limit_bytes=60 * 1024 * 1024
        ),
    )(left, middle.reshape(2, rows // 2, -1), right.reshape(2, rows // 2, -1))


def solution(mesh):
    return jax.shard_map(
        per_device,
        mesh=mesh,
        in_specs=(P("row", ("col", "layer")), P("row", "col"), P("row", "col")),
        out_specs=P("row", ("col", "layer")),
        check_vma=False,
    )
```

```python
import jax
import jax.numpy as jnp
from jax import lax
from jax.experimental import pallas as pl
from jax.experimental.pallas import tpu as pltpu
from jax.sharding import PartitionSpec as P

MESH = pl.DeviceIdType.MESH
BF16 = jnp.bfloat16
TM = 256
TILES = 1024 // TM
UNITS = (4, 8)

STAGES = [(0, 0), (0, 1), (0, 2), (0, 3), (1, 0), (1, 1), (1, 2), (1, 3)]

ORDER = [
    (1, 0), (0, 0), (1, 1), (0, 1), (1, 2), (0, 2), (1, 3), (2, 0), (0, 3), (2, 1), (3, 0),
    (2, 2), (3, 1), (2, 3), (3, 2), (4, 0), (3, 3), (4, 1), (5, 0), (4, 2), (5, 1), (4, 3),
    (6, 0), (5, 2), (6, 1), (5, 3), (7, 0), (6, 2), (7, 1), (6, 3), (7, 2), (7, 3),
]
LAST = 7


def rem(a, n):
    return lax.rem(a + 4 * n, jnp.int32(n))


def kernel(left, middle, right, out, A, B, Bx, own_sum, send, recv,
           zS, zR, xS, xR, dS, dR, cS, cR, hS, hR, wS, wR, lS):
    z = lax.axis_index("row")
    col = lax.axis_index("col")
    h = lax.axis_index("layer")
    c = lax.rem(col, 2)
    x = lax.rem(lax.div(col, 2), 4)
    lo = lax.div(col, 8)
    y = h * 2 + lo

    def dev(zz=None, xx=None, yy=None, cc=None):
        zz = z if zz is None else zz
        xx = x if xx is None else xx
        yy = y if yy is None else yy
        cc = c if cc is None else cc
        return (zz, lax.rem(yy, 2) * 8 + xx * 2 + cc, lax.div(yy, 2))

    z_to = [dev(zz=rem(z + 1, 8)), dev(zz=rem(z - 1, 8))]
    x_to = [dev(xx=rem(x + 1, 4)), dev(xx=rem(x - 1, 4))]
    y_of = [dev(yy=rem(y + d, 4)) for d in (1, 2, 3)]
    pair = dev(yy=h * 2 + 1 - lo)
    yt = h * 2 + 1 - lo
    core = dev(cc=1 - c)

    barrier = pltpu.get_barrier_semaphore()
    for peer in z_to + x_to + y_of + [core]:
        pl.semaphore_signal(barrier, inc=1, device_id=peer, device_id_type=MESH)

    def m128(v):
        return pl.multiple_of(v, 128)

    def zpos(zz):
        return lax.rem(zz, 4) * 2 + lax.div(zz, 4)

    def local(src, dst, sem):
        return pltpu.make_async_copy(src, dst, sem)

    def remote(src, dst, ssem, rsem, to):
        return pltpu.make_async_remote_copy(
            src_ref=src, dst_ref=dst, send_sem=ssem, recv_sem=rsem, device_id=to, device_id_type=MESH
        )

    ymod = lambda v: rem(v, 4)

    def own_rows(p, j, cols_from, width, cols_to, ywho):
        src = (middle, right)[p].at[:, pl.ds(m128(ywho * 128), 128), pl.ds(m128(cols_from), width)]
        dst = B.at[p, j, :, zpos(z), :, pl.ds(cols_to, width)]
        return src, dst

    def own_parts(yw, l_src):
        own = [
            (0, 1, ymod(yw + 1) * 128, 128, 0),
            (0, 1, ymod(yw + 3) * 128, 128, 128),
            (0, 0, ymod(yw + 2) * 128, 128, m128(l_src * 128)),
            (0, 3, yw * 128, 128, m128(l_src * 128)),
            (1, 0, lax.div(ymod(yw + 2), 2) * 256, 256, 0),
            (1, 3, lax.div(yw, 2) * 256, 256, 0),
        ]
        hop = [
            (0, 0, ymod(yw + 2) * 128, 128, m128(l_src * 128)),
            (0, 2, ymod(yw + 1) * 128, 128, 0),
            (0, 2, ymod(yw + 3) * 128, 128, 128),
            (0, 3, yw * 128, 128, m128(l_src * 128)),
            (1, 1, lax.div(ymod(yw + 1), 2) * 256, 128, 0),
            (1, 1, lax.div(ymod(yw + 3), 2) * 256, 128, 128),
            (1, 2, lax.div(ymod(yw + 1), 2) * 256 + 128, 128, 0),
            (1, 2, lax.div(ymod(yw + 3), 2) * 256 + 128, 128, 128),
        ]
        return own, hop

    own, _ = own_parts(y, lo)
    _, hop_out = own_parts(yt, lo)
    _, hop_in = own_parts(y, 1 - lo)
    own_copies = [local(*own_rows(p, j, f, w, t, y), lS.at[i]) for i, (p, j, f, w, t) in enumerate(own)]
    hop_sends = [
        remote(*own_rows(p, j, f, w, t, yt), hS, hR.at[i], pair) for i, (p, j, f, w, t) in enumerate(hop_out)
    ]
    hop_recvs = [
        remote(*own_rows(p, j, f, w, t, y), hS, hR.at[i], pair) for i, (p, j, f, w, t) in enumerate(hop_in)
    ]

    def strip(cc, xx):
        return (cc * 4 + xx) * 256

    def xregion(p, cc, xx, u):
        if p == 0:
            half = lo if u < 2 else 1 - lo
            return A.at[0, pl.ds((u % 2) * 512, 512), pl.ds(m128(strip(cc, xx) + half * 128), 128)]
        return A.at[1, pl.ds(pl.multiple_of(u * 128, 128), 128), pl.ds(m128(strip(cc, xx)), 256)]

    left_copy = local(
        left.at[:, pl.ds(m128(lo * 128), 128)],
        A.at[0, :, pl.ds(m128(strip(c, x) + lo * 128), 128)],
        lS.at[6],
    )
    swaps = [
        remote(
            left.at[pl.ds(u * 512, 512), pl.ds(m128((1 - lo) * 128), 128)],
            A.at[0, pl.ds(u * 512, 512), pl.ds(m128(strip(c, x) + lo * 128), 128)],
            wS, wR.at[u], pair,
        )
        for u in range(2)
    ]
    swap_recvs = [
        remote(
            left.at[pl.ds(u * 512, 512), pl.ds(m128((1 - lo) * 128), 128)],
            A.at[0, pl.ds(u * 512, 512), pl.ds(m128(strip(c, x) + (1 - lo) * 128), 128)],
            wS, wR.at[u], pair,
        )
        for u in range(2)
    ]

    left_copy.start()
    for i in range(6):
        own_copies[i].start()

    for half in range(2):
        B[1, 3, half, zpos(rem(z + 4, 8))] = jnp.zeros((128, 256), BF16)

    pl.semaphore_wait(barrier, 8)

    hop_sends[0].start()
    for u in range(2):
        swaps[u].start()
    for i in range(1, 8):
        hop_sends[i].start()

    OWN_OF = {(0, 0): [2], (0, 1): [0, 1], (0, 2): [], (0, 3): [3], (1, 0): [4], (1, 1): [], (1, 2): [], (1, 3): [5]}
    HOP_OF = {(0, 0): [0], (0, 1): [], (0, 2): [1, 2], (0, 3): [3], (1, 0): [], (1, 1): [4, 5], (1, 2): [6, 7], (1, 3): []}

    def z_copy(s, d, minor, level, arriving):
        p, j = STAGES[s]
        sign = -1 if d == 0 else 1
        half = d if minor == 0 else 1 - d
        block = rem(z + sign * (level + (1 if arriving else 0)), 8)
        ref = B.at[p, j, half, zpos(block)]
        k = level + (4 if minor else 0)
        if s == LAST and level == 3:
            return remote(ref, Bx.at[half], zS.at[p], zR.at[d, s, k], z_to[d])
        return remote(ref, ref, zS.at[p], zR.at[d, s, k], z_to[d])

    def z_tick(s, level):
        if level == 0:
            for i in OWN_OF[STAGES[s]]:
                own_copies[i].wait()
            for i in HOP_OF[STAGES[s]]:
                hop_recvs[i].wait_recv()
        for minor in range(2):
            if minor == 1 and level == 3:
                continue
            for d in range(2):
                if level > 0:
                    z_copy(s, d, minor, level - 1, True).wait_recv()
                z_copy(s, d, minor, level, False).start()

    def z_minor(s):
        for d in range(2):
            z_copy(s, d, 1, 2, True).wait_recv()

    def z_major(s):
        for d in range(2):
            z_copy(s, d, 0, 3, True).wait_recv()

    def z_last(s):
        z_minor(s)
        z_major(s)

    def x_copy(p, d, u, forward, arriving):
        sign = -1 if d == 0 else 1
        away = (1 if forward else 0) + (1 if arriving else 0)
        ref = xregion(p, c, rem(x + sign * away, 4), u)
        k = UNITS[p] + u // 2 if forward else u
        return remote(ref, ref, xS.at[p], xR.at[p * 12 + d * (6, 12)[p] + k], x_to[d])

    def x_forward(p, d, u):
        x_copy(p, d, u, False, True).wait_recv()
        x_copy(p, d, u, True, False).start()

    def d_copy(p, away, g, arriving):
        cc, xx = 1 - c if arriving else c, rem(x + away, 4)
        if p == 0:
            half = lo if g == 0 else 1 - lo
            ref = A.at[0, :, pl.ds(m128(strip(cc, xx) + half * 128), 128)]
        else:
            ref = A.at[1, pl.ds(pl.multiple_of(g * TM, TM), TM), pl.ds(m128(strip(cc, xx)), 256)]
        return remote(ref, ref, dS.at[p], dR.at[p * 8 + away * (2, 4)[p] + g], core)

    def d_all(p, gs):
        for away in range(4):
            for g in gs:
                d_copy(p, away, g, True).wait_recv()

    def x_send_tile(t):
        for u in range(2 * t, 2 * t + 2):
            x_copy(1, 0, u, False, False).start()
            x_copy(1, 1, 4 * t + 1 - u, False, False).start()

    def c_copies(p, j, t, arriving):
        rows = pl.ds(t * TM, TM)
        if j == 0:
            return [remote(send.at[p, 0, rows], recv.at[p, 1, rows], cS.at[p], cR.at[p, 0, t], y_of[1])]
        made = []
        for q in range(2):
            if p == 0:
                which = lo if (j == 1) != arriving else 1 - lo
                place = m128(which * 128)
            else:
                place = (j - 1) * 128
            k = 1 + (j - 1) * 2 + q
            made.append(
                remote(
                    send.at[p, j, rows, pl.ds(q * 128, 128)],
                    recv.at[p, 2 * q, rows, pl.ds(place, 128)],
                    cS.at[p], cR.at[p, k, t], y_of[2 * q],
                )
            )
        return made

    def compute(s, t0, t1):
        p, j = STAGES[s]

        def body(t, carry):
            rows = pl.ds(pl.multiple_of(t * TM, TM), TM)
            acc = jnp.dot(A[p, rows, :], B[p, j].reshape(2048, 256), preferred_element_type=jnp.float32)
            if j < 3:
                send[p, j, rows, :] = acc.astype(BF16)
                for copy in c_copies(p, j, t, False):
                    copy.start()
                return carry
            if s == LAST:
                own_sum[rows, :] = acc
                return carry
            finish(p, t, rows, acc)
            return carry

        lax.fori_loop(t0, t1, body, 0)

    def finish_last(t0, t1):
        def body(t, carry):
            rows = pl.ds(pl.multiple_of(t * TM, TM), TM)
            far = zpos(rem(z + 4, 8))
            piece = jnp.concatenate(
                [A[1, rows, pl.ds(m128((half * 8 + far) * 128), 128)] for half in range(2)], axis=1
            )
            acc = jnp.dot(piece, Bx[...].reshape(256, 256), preferred_element_type=jnp.float32)
            finish(1, t, rows, own_sum[rows, :] + acc)
            return carry

        lax.fori_loop(t0, t1, body, 0)

    def finish(p, t, rows, acc):
        if True:
            for jj in range(3):
                for copy in c_copies(p, jj, t, True):
                    copy.wait_recv()
            for d in range(3):
                acc = acc + recv[p, d, rows, :].astype(jnp.float32)
            if p == 0:
                A[1, rows, pl.ds(m128(strip(c, x)), 256)] = acc.astype(BF16)
                d_copy(1, 0, t, False).start()
            else:
                out[rows, :] = acc.astype(BF16)

    def x_start(u):
        if u == 0:
            left_copy.wait()
        if u >= 2:
            swap_recvs[u - 2].wait_recv()
        for d in range(2):
            x_copy(0, d, u, False, False).start()
        if u % 2 == 1:
            d_copy(0, 0, u // 2, False).start()

    def x_forwards(p, us):
        for u in us:
            x_forward(p, u % 2, u)

    def x_rest(p, g):
        for u in (2 * g, 2 * g + 1):
            x_copy(p, 1 - u % 2, u, False, True).wait_recv()
        for away in (1, 3):
            d_copy(p, away, g, False).start()

    def x_far(p, g):
        for u in (2 * g, 2 * g + 1):
            x_copy(p, u % 2, u, True, True).wait_recv()
        d_copy(p, 2, g, False).start()

    def do(f, *args):
        return lambda: f(*args)

    ACTIONS = {
        0: [do(x_start, 0), do(x_start, 1)],
        1: [do(x_forwards, 0, (0, 1))],
        2: [do(x_start, 2), do(x_rest, 0, 0)],
        3: [do(x_start, 3), do(x_far, 0, 0)],
        4: [do(x_forwards, 0, (2,))],
        5: [do(x_forwards, 0, (3,))],
        7: [do(x_rest, 0, 1)],
        8: [do(x_far, 0, 1), do(d_all, 0, (0, 1))],
        10: [do(z_last, 1), do(compute, 1, 0, 4), do(z_last, 0), do(compute, 0, 0, 2)],
        11: [do(compute, 0, 2, 4)],
        15: [do(z_last, 2), do(compute, 2, 0, 4)],
        18: [do(z_last, 3)],
        19: [do(compute, 3, 0, 1), do(x_send_tile, 0), do(compute, 3, 1, 2), do(x_send_tile, 1), do(compute, 3, 2, 4)],
        20: [do(x_forwards, 1, (0, 1)), do(x_send_tile, 2)],
        22: [do(x_forwards, 1, (2, 3)), do(x_send_tile, 3), do(x_rest, 1, 0), do(x_rest, 1, 1)],
        23: [do(x_far, 1, 0), do(x_forwards, 1, (4, 5)), do(z_last, 4), do(d_all, 1, (0,)), do(compute, 4, 0, 1)],
        24: [do(x_rest, 1, 2), do(x_far, 1, 1), do(d_all, 1, (1,)), do(compute, 4, 1, 2)],
        26: [do(x_forwards, 1, (6, 7)), do(x_rest, 1, 3), do(x_far, 1, 2), do(d_all, 1, (2,)),
             do(compute, 4, 2, 3), do(x_far, 1, 3)],
        27: [do(d_all, 1, (3,)), do(compute, 4, 3, 4), do(z_last, 5), do(compute, 5, 0, 4)],
        30: [do(z_last, 6), do(compute, 6, 0, 3)],
        31: [do(compute, 6, 3, 4), do(z_minor, 7), do(compute, 7, 0, 4), do(z_major, 7), do(finish_last, 0, 4)],
    }
    for i, (s, level) in enumerate(ORDER):
        z_tick(s, level)
        for action in ACTIONS.get(i, ()):
            action()

    def all_sent(ref, sem):
        remote(ref, ref, sem, sem, core).wait_send()

    all_sent(B.at[0, 0, 0], hS)
    all_sent(A.at[0, pl.ds(0, 64)], wS)
    for p in range(2):
        all_sent(B.at[p, :, :, pl.ds(0, 7)], zS.at[p])
        all_sent(A.at[p, pl.ds(0, 384)], xS.at[p])
        all_sent(A.at[p, pl.ds(0, 512)], dS.at[p])
        all_sent(send.at[p], cS.at[p])


def per_device(left, middle, right):
    rows, width = left.shape
    dma = pltpu.SemaphoreType.DMA
    return pl.pallas_call(
        kernel,
        out_shape=jax.ShapeDtypeStruct((rows, width), BF16),
        in_specs=[pl.BlockSpec(memory_space=pl.ANY)] * 3,
        out_specs=pl.BlockSpec(memory_space=pltpu.VMEM),
        scratch_shapes=[
            pltpu.VMEM((2, 1024, 2048), BF16),
            pltpu.VMEM((2, 4, 2, 8, 128, 256), BF16),
            pltpu.VMEM((2, 128, 256), BF16),
            pltpu.VMEM((1024, 256), jnp.float32),
            pltpu.VMEM((2, 3, 1024, 256), BF16),
            pltpu.VMEM((2, 3, 1024, 256), BF16),
            dma((2,)), dma((2, 8, 7)),
            dma((2,)), dma((36,)),
            dma((2,)), dma((24,)),
            dma((2,)), dma((2, 5, TILES)),
            dma(()), dma((8,)),
            dma(()), dma((2,)),
            dma((7,)),
        ],
        compiler_params=pltpu.CompilerParams(
            collective_id=0, has_side_effects=True, vmem_limit_bytes=int(62 * 1024 * 1024)
        ),
    )(left, middle.reshape(2, rows // 2, -1), right.reshape(2, rows // 2, -1))


def solution(mesh):
    return jax.shard_map(
        per_device,
        mesh=mesh,
        in_specs=(P("row", ("col", "layer")), P("row", "col"), P("row", "col")),
        out_specs=P("row", ("col", "layer")),
        check_vma=False,
    )
```

```python
import jax
import jax.numpy as jnp
from jax import lax
from jax.experimental import pallas as pl
from jax.experimental.pallas import tpu as pltpu
from jax.sharding import PartitionSpec as P

MESH = pl.DeviceIdType.MESH
BF16 = jnp.bfloat16
TM = 256
TILES = 1024 // TM
UNITS = (4, 8)

STAGES = [(0, 0), (0, 1), (0, 2), (0, 3), (1, 0), (1, 1), (1, 2), (1, 3)]

ORDER = [
    (1, 0), (0, 0), (1, 1), (0, 1), (1, 2), (0, 2), (1, 3), (2, 0), (0, 3), (2, 1), (3, 0),
    (2, 2), (3, 1), (2, 3), (3, 2), (3, 3), (4, 0), (4, 1), (5, 0), (4, 2), (5, 1), (4, 3),
    (6, 0), (5, 2), (6, 1), (5, 3), (6, 2), (7, 0), (6, 3), (7, 1), (7, 2), (7, 3),
]
PARTS = (1, 1, 1, 2, 2, 1, 1, 2)
FIRST = [sum(14 * n for n in PARTS[:s]) for s in range(9)]
LAST = 7


def rem(a, n):
    return lax.rem(a + 4 * n, jnp.int32(n))


def kernel(left, middle, right, out, A, B, Bx, own_sum, send, recv,
           zS, zR, xS, xR, dS, dR, cS, cR, hS, hR, wS, wR, lS):
    z = lax.axis_index("row")
    col = lax.axis_index("col")
    h = lax.axis_index("layer")
    c = lax.rem(col, 2)
    x = lax.rem(lax.div(col, 2), 4)
    lo = lax.div(col, 8)
    y = h * 2 + lo

    def dev(zz=None, xx=None, yy=None, cc=None):
        zz = z if zz is None else zz
        xx = x if xx is None else xx
        yy = y if yy is None else yy
        cc = c if cc is None else cc
        return (zz, lax.rem(yy, 2) * 8 + xx * 2 + cc, lax.div(yy, 2))

    z_to = [dev(zz=rem(z + 1, 8)), dev(zz=rem(z - 1, 8))]
    x_to = [dev(xx=rem(x + 1, 4)), dev(xx=rem(x - 1, 4))]
    y_of = [dev(yy=rem(y + d, 4)) for d in (1, 2, 3)]
    pair = dev(yy=h * 2 + 1 - lo)
    yt = h * 2 + 1 - lo
    core = dev(cc=1 - c)

    barrier = pltpu.get_barrier_semaphore()
    for peer in z_to + x_to + y_of + [core]:
        pl.semaphore_signal(barrier, inc=1, device_id=peer, device_id_type=MESH)

    def m128(v):
        return pl.multiple_of(v, 128)

    def zpos(zz):
        return lax.rem(zz, 4) * 2 + lax.div(zz, 4)

    def local(src, dst, sem):
        return pltpu.make_async_copy(src, dst, sem)

    def remote(src, dst, ssem, rsem, to):
        return pltpu.make_async_remote_copy(
            src_ref=src, dst_ref=dst, send_sem=ssem, recv_sem=rsem, device_id=to, device_id_type=MESH
        )

    ymod = lambda v: rem(v, 4)

    def own_rows(p, j, cols_from, width, cols_to, ywho):
        src = (middle, right)[p].at[:, pl.ds(m128(ywho * 128), 128), pl.ds(m128(cols_from), width)]
        dst = B.at[p, j, :, zpos(z), :, pl.ds(cols_to, width)]
        return src, dst

    def own_parts(yw, l_src):
        own = [
            (0, 1, ymod(yw + 1) * 128, 128, 0),
            (0, 1, ymod(yw + 3) * 128, 128, 128),
            (0, 0, ymod(yw + 2) * 128, 128, m128(l_src * 128)),
            (0, 3, yw * 128, 128, m128(l_src * 128)),
            (1, 0, lax.div(ymod(yw + 2), 2) * 256, 256, 0),
            (1, 3, lax.div(yw, 2) * 256, 256, 0),
        ]
        hop = [
            (0, 0, ymod(yw + 2) * 128, 128, m128(l_src * 128)),
            (0, 2, ymod(yw + 1) * 128, 128, 0),
            (0, 2, ymod(yw + 3) * 128, 128, 128),
            (0, 3, yw * 128, 128, m128(l_src * 128)),
            (1, 1, lax.div(ymod(yw + 1), 2) * 256, 128, 0),
            (1, 1, lax.div(ymod(yw + 3), 2) * 256, 128, 128),
            (1, 2, lax.div(ymod(yw + 1), 2) * 256 + 128, 128, 0),
            (1, 2, lax.div(ymod(yw + 3), 2) * 256 + 128, 128, 128),
        ]
        return own, hop

    own, _ = own_parts(y, lo)
    _, hop_out = own_parts(yt, lo)
    _, hop_in = own_parts(y, 1 - lo)
    own_copies = [local(*own_rows(p, j, f, w, t, y), lS.at[i]) for i, (p, j, f, w, t) in enumerate(own)]
    hop_sends = [
        remote(*own_rows(p, j, f, w, t, yt), hS, hR.at[i], pair) for i, (p, j, f, w, t) in enumerate(hop_out)
    ]
    hop_recvs = [
        remote(*own_rows(p, j, f, w, t, y), hS, hR.at[i], pair) for i, (p, j, f, w, t) in enumerate(hop_in)
    ]

    def strip(cc, xx):
        return (cc * 4 + xx) * 256

    def xregion(p, cc, xx, u):
        if p == 0:
            half = lo if u < 2 else 1 - lo
            return A.at[0, pl.ds((u % 2) * 512, 512), pl.ds(m128(strip(cc, xx) + half * 128), 128)]
        return A.at[1, pl.ds(pl.multiple_of(u * 128, 128), 128), pl.ds(m128(strip(cc, xx)), 256)]

    left_copy = local(
        left.at[:, pl.ds(m128(lo * 128), 128)],
        A.at[0, :, pl.ds(m128(strip(c, x) + lo * 128), 128)],
        lS.at[6],
    )
    swaps = [
        remote(
            left.at[pl.ds(u * 512, 512), pl.ds(m128((1 - lo) * 128), 128)],
            A.at[0, pl.ds(u * 512, 512), pl.ds(m128(strip(c, x) + lo * 128), 128)],
            wS, wR.at[u], pair,
        )
        for u in range(2)
    ]
    swap_recvs = [
        remote(
            left.at[pl.ds(u * 512, 512), pl.ds(m128((1 - lo) * 128), 128)],
            A.at[0, pl.ds(u * 512, 512), pl.ds(m128(strip(c, x) + (1 - lo) * 128), 128)],
            wS, wR.at[u], pair,
        )
        for u in range(2)
    ]

    left_copy.start()
    for i in range(6):
        own_copies[i].start()

    for half in range(2):
        B[1, 3, half, zpos(rem(z + 4, 8))] = jnp.zeros((128, 256), BF16)

    pl.semaphore_wait(barrier, 8)

    hop_sends[0].start()
    for u in range(2):
        swaps[u].start()
    for i in range(1, 8):
        hop_sends[i].start()

    OWN_OF = {(0, 0): [2], (0, 1): [0, 1], (0, 2): [], (0, 3): [3], (1, 0): [4], (1, 1): [], (1, 2): [], (1, 3): [5]}
    HOP_OF = {(0, 0): [0], (0, 1): [], (0, 2): [1, 2], (0, 3): [3], (1, 0): [], (1, 1): [4, 5], (1, 2): [6, 7], (1, 3): []}

    def z_copy(s, d, minor, level, part, arriving):
        p, j = STAGES[s]
        sign = -1 if d == 0 else 1
        half = d if minor == 0 else 1 - d
        block = rem(z + sign * (level + (1 if arriving else 0)), 8)
        rows = pl.ds(part * (128 // PARTS[s]), 128 // PARTS[s])
        src = B.at[p, j, half, zpos(block), rows]
        dst = Bx.at[half, rows] if s == LAST and level == 3 else src
        k = FIRST[s] + (d * 7 + level + (4 if minor else 0)) * PARTS[s] + part
        return remote(src, dst, zS.at[p], zR.at[k], z_to[d])

    def z_tick(s, level):
        if level == 0:
            for i in OWN_OF[STAGES[s]]:
                own_copies[i].wait()
            for i in HOP_OF[STAGES[s]]:
                hop_recvs[i].wait_recv()
        for minor in range(1 if level == 3 else 2):
            for part in range(PARTS[s]):
                for d in range(2):
                    if level > 0:
                        z_copy(s, d, minor, level - 1, part, True).wait_recv()
                    z_copy(s, d, minor, level, part, False).start()

    def z_minor(s):
        for part in range(PARTS[s]):
            for d in range(2):
                z_copy(s, d, 1, 2, part, True).wait_recv()

    def z_major(s):
        for part in range(PARTS[s]):
            for d in range(2):
                z_copy(s, d, 0, 3, part, True).wait_recv()

    def z_last(s):
        z_minor(s)
        z_major(s)

    def x_copy(p, d, u, forward, arriving):
        sign = -1 if d == 0 else 1
        away = (1 if forward else 0) + (1 if arriving else 0)
        ref = xregion(p, c, rem(x + sign * away, 4), u)
        k = UNITS[p] + u // 2 if forward else u
        return remote(ref, ref, xS.at[p], xR.at[p * 12 + d * (6, 12)[p] + k], x_to[d])

    def x_forward(p, d, u):
        x_copy(p, d, u, False, True).wait_recv()
        x_copy(p, d, u, True, False).start()

    def d_copy(p, away, g, arriving):
        cc, xx = 1 - c if arriving else c, rem(x + away, 4)
        if p == 0:
            half = lo if g == 0 else 1 - lo
            ref = A.at[0, :, pl.ds(m128(strip(cc, xx) + half * 128), 128)]
        else:
            ref = A.at[1, pl.ds(pl.multiple_of(g * TM, TM), TM), pl.ds(m128(strip(cc, xx)), 256)]
        return remote(ref, ref, dS.at[p], dR.at[p * 8 + away * (2, 4)[p] + g], core)

    def d_all(p, gs):
        for away in range(4):
            for g in gs:
                d_copy(p, away, g, True).wait_recv()

    def x_send_tile(t):
        for u in range(2 * t, 2 * t + 2):
            x_copy(1, 0, u, False, False).start()
            x_copy(1, 1, 4 * t + 1 - u, False, False).start()

    def c_copies(p, j, t, arriving):
        rows = pl.ds(t * TM, TM)
        if j == 0:
            return [remote(send.at[p, 0, rows], recv.at[p, 1, rows], cS.at[p], cR.at[p, 0, t], y_of[1])]
        made = []
        for q in range(2):
            if p == 0:
                which = lo if (j == 1) != arriving else 1 - lo
                place = m128(which * 128)
            else:
                place = (j - 1) * 128
            k = 1 + (j - 1) * 2 + q
            made.append(
                remote(
                    send.at[p, j, rows, pl.ds(q * 128, 128)],
                    recv.at[p, 2 * q, rows, pl.ds(place, 128)],
                    cS.at[p], cR.at[p, k, t], y_of[2 * q],
                )
            )
        return made

    def compute(s, t0, t1):
        p, j = STAGES[s]

        def body(t, carry):
            rows = pl.ds(t * TM if isinstance(t, int) else pl.multiple_of(t * TM, TM), TM)
            acc = jnp.dot(A[p, rows, :], B[p, j].reshape(2048, 256), preferred_element_type=jnp.float32)
            if j < 3:
                send[p, j, rows, :] = acc.astype(BF16)
                for copy in c_copies(p, j, t, False):
                    copy.start()
                return carry
            if s == LAST:
                own_sum[rows, :] = acc
                return carry
            finish(p, t, rows, acc)
            return carry

        if s == LAST:
            for t in range(t0, t1):
                body(t, 0)
            return
        lax.fori_loop(t0, t1, body, 0)

    def finish_last(t0, t1):
        def body(t, carry):
            rows = pl.ds(t * TM if isinstance(t, int) else pl.multiple_of(t * TM, TM), TM)
            far = zpos(rem(z + 4, 8))
            piece = jnp.concatenate(
                [A[1, rows, pl.ds(m128((half * 8 + far) * 128), 128)] for half in range(2)], axis=1
            )
            acc = jnp.dot(piece, Bx[...].reshape(256, 256), preferred_element_type=jnp.float32)
            finish(1, t, rows, own_sum[rows, :] + acc)
            return carry

        lax.fori_loop(t0, t1, body, 0)

    def finish(p, t, rows, acc):
        if True:
            for jj in range(3):
                for copy in c_copies(p, jj, t, True):
                    copy.wait_recv()
            for d in range(3):
                acc = acc + recv[p, d, rows, :].astype(jnp.float32)
            if p == 0:
                A[1, rows, pl.ds(m128(strip(c, x)), 256)] = acc.astype(BF16)
                d_copy(1, 0, t, False).start()
            else:
                out[rows, :] = acc.astype(BF16)

    def x_start(u):
        if u == 0:
            left_copy.wait()
        if u >= 2:
            swap_recvs[u - 2].wait_recv()
        for d in range(2):
            x_copy(0, d, u, False, False).start()
        if u % 2 == 1:
            d_copy(0, 0, u // 2, False).start()

    def x_forwards(p, us):
        for u in us:
            x_forward(p, u % 2, u)

    def x_rest(p, g):
        for u in (2 * g, 2 * g + 1):
            x_copy(p, 1 - u % 2, u, False, True).wait_recv()
        for away in (1, 3):
            d_copy(p, away, g, False).start()

    def x_far(p, g):
        for u in (2 * g, 2 * g + 1):
            x_copy(p, u % 2, u, True, True).wait_recv()
        d_copy(p, 2, g, False).start()

    def do(f, *args):
        return lambda: f(*args)

    ACTIONS = {
        0: [do(x_start, 0), do(x_start, 1)],
        1: [do(x_forwards, 0, (0, 1))],
        2: [do(x_start, 2), do(x_rest, 0, 0)],
        3: [do(x_start, 3), do(x_far, 0, 0)],
        4: [do(x_forwards, 0, (2,))],
        5: [do(x_forwards, 0, (3,))],
        7: [do(x_rest, 0, 1)],
        8: [do(x_far, 0, 1)],
        10: [do(z_last, 1), do(d_all, 0, (0, 1)), do(compute, 1, 0, 4), do(z_last, 0), do(compute, 0, 0, 2)],
        11: [do(compute, 0, 2, 4)],
        14: [do(z_last, 2), do(compute, 2, 0, 1)],
        16: [do(compute, 2, 1, 4)],
        18: [do(z_last, 3), do(compute, 3, 0, 1), do(x_send_tile, 0), do(compute, 3, 1, 2), do(x_send_tile, 1),
             do(compute, 3, 2, 3)],
        19: [do(compute, 3, 3, 4), do(x_forwards, 1, (0, 1)), do(x_send_tile, 2)],
        20: [do(x_forwards, 1, (2, 3)), do(x_send_tile, 3), do(x_rest, 1, 0)],
        22: [do(x_rest, 1, 1), do(x_far, 1, 0)],
        23: [do(x_forwards, 1, (4, 5)), do(z_last, 4), do(d_all, 1, (0,)), do(compute, 4, 0, 1), do(x_far, 1, 1)],
        24: [do(x_rest, 1, 2), do(x_forwards, 1, (6, 7)), do(d_all, 1, (1,)), do(compute, 4, 1, 2)],
        25: [do(x_far, 1, 2)],
        26: [do(x_rest, 1, 3)],
        27: [do(d_all, 1, (2,)), do(compute, 4, 2, 3), do(x_far, 1, 3), do(z_last, 5), do(compute, 5, 0, 2), do(d_all, 1, (3,)),
             do(compute, 4, 3, 4), do(compute, 5, 2, 4)],
        29: [do(z_last, 6), do(compute, 6, 0, 1)],
        30: [do(compute, 6, 1, 4)],
        31: [do(z_minor, 7), do(compute, 7, 0, 4), do(z_major, 7), do(finish_last, 0, 4)],
    }
    for i, (s, level) in enumerate(ORDER):
        z_tick(s, level)
        for action in ACTIONS.get(i, ()):
            action()

    def all_sent(ref, sem):
        remote(ref, ref, sem, sem, core).wait_send()

    all_sent(B.at[0, 0, 0], hS)
    all_sent(A.at[0, pl.ds(0, 64)], wS)
    for p in range(2):
        all_sent(B.at[p, :, :, pl.ds(0, 7)], zS.at[p])
        all_sent(A.at[p, pl.ds(0, 384)], xS.at[p])
        all_sent(A.at[p, pl.ds(0, 512)], dS.at[p])
        all_sent(send.at[p], cS.at[p])


def per_device(left, middle, right):
    rows, width = left.shape
    dma = pltpu.SemaphoreType.DMA
    return pl.pallas_call(
        kernel,
        out_shape=jax.ShapeDtypeStruct((rows, width), BF16),
        in_specs=[pl.BlockSpec(memory_space=pl.ANY)] * 3,
        out_specs=pl.BlockSpec(memory_space=pltpu.VMEM),
        scratch_shapes=[
            pltpu.VMEM((2, 1024, 2048), BF16),
            pltpu.VMEM((2, 4, 2, 8, 128, 256), BF16),
            pltpu.VMEM((2, 128, 256), BF16),
            pltpu.VMEM((1024, 256), jnp.float32),
            pltpu.VMEM((2, 3, 1024, 256), BF16),
            pltpu.VMEM((2, 3, 1024, 256), BF16),
            dma((2,)), dma((FIRST[8],)),
            dma((2,)), dma((36,)),
            dma((2,)), dma((24,)),
            dma((2,)), dma((2, 5, TILES)),
            dma(()), dma((8,)),
            dma(()), dma((2,)),
            dma((7,)),
        ],
        compiler_params=pltpu.CompilerParams(
            collective_id=0, has_side_effects=True, vmem_limit_bytes=int(52 * 1024 * 1024)
        ),
    )(left, middle.reshape(2, rows // 2, -1), right.reshape(2, rows // 2, -1))


def solution(mesh):
    return jax.shard_map(
        per_device,
        mesh=mesh,
        in_specs=(P("row", ("col", "layer")), P("row", "col"), P("row", "col")),
        out_specs=P("row", ("col", "layer")),
        check_vma=False,
    )
```

```python
import jax
import jax.numpy as jnp
from jax import lax
from jax.experimental import pallas as pl
from jax.experimental.pallas import tpu as pltpu
from jax.sharding import PartitionSpec as P

MESH = pl.DeviceIdType.MESH
BF16 = jnp.bfloat16
TM = 256
TILES = 1024 // TM
UNITS = (4, 8)

STAGES = [(0, 0), (0, 1), (0, 2), (0, 3), (1, 0), (1, 1), (1, 2), (1, 3)]

ORDER = [
    (1, 0), (0, 0), (1, 1), (0, 1), (1, 2), (0, 2), (1, 3), (2, 0), (0, 3), (2, 1), (3, 0),
    (2, 2), (3, 1), (2, 3), (3, 2), (3, 3), (4, 0), (4, 1), (5, 0), (4, 2), (5, 1), (4, 3),
    (6, 0), (5, 2), (6, 1), (5, 3), (7, 0), (6, 2), (7, 1), (6, 3), (7, 2), (7, 3),
]
PARTS = (1, 1, 1, 2, 2, 1, 1, 2)
FIRST = [sum(14 * n for n in PARTS[:s]) for s in range(9)]
LAST = 7


def rem(a, n):
    return lax.rem(a + 4 * n, jnp.int32(n))


def kernel(left, middle, right, out, A, B, Bx, own_sum, send, recv, relay,
           zS, zR, xS, xR, dS, dR, cS, cR, hS, hR, wS, wR, lS):
    z = lax.axis_index("row")
    col = lax.axis_index("col")
    h = lax.axis_index("layer")
    c = lax.rem(col, 2)
    x = lax.rem(lax.div(col, 2), 4)
    lo = lax.div(col, 8)
    y = h * 2 + lo

    def dev(zz=None, xx=None, yy=None, cc=None):
        zz = z if zz is None else zz
        xx = x if xx is None else xx
        yy = y if yy is None else yy
        cc = c if cc is None else cc
        return (zz, lax.rem(yy, 2) * 8 + xx * 2 + cc, lax.div(yy, 2))

    z_to = [dev(zz=rem(z + 1, 8)), dev(zz=rem(z - 1, 8))]
    x_to = [dev(xx=rem(x + 1, 4)), dev(xx=rem(x - 1, 4))]
    y_of = [dev(yy=rem(y + d, 4)) for d in (1, 2, 3)]
    pair = dev(yy=h * 2 + 1 - lo)
    yt = h * 2 + 1 - lo
    core = dev(cc=1 - c)

    barrier = pltpu.get_barrier_semaphore()
    for peer in z_to + x_to + y_of + [core]:
        pl.semaphore_signal(barrier, inc=1, device_id=peer, device_id_type=MESH)

    def m128(v):
        return pl.multiple_of(v, 128)

    def zpos(zz):
        return lax.rem(zz, 4) * 2 + lax.div(zz, 4)

    def local(src, dst, sem):
        return pltpu.make_async_copy(src, dst, sem)

    def remote(src, dst, ssem, rsem, to):
        return pltpu.make_async_remote_copy(
            src_ref=src, dst_ref=dst, send_sem=ssem, recv_sem=rsem, device_id=to, device_id_type=MESH
        )

    ymod = lambda v: rem(v, 4)

    def own_rows(p, j, cols_from, width, cols_to, ywho):
        src = (middle, right)[p].at[:, pl.ds(m128(ywho * 128), 128), pl.ds(m128(cols_from), width)]
        dst = B.at[p, j, :, zpos(z), :, pl.ds(cols_to, width)]
        return src, dst

    def own_parts(yw, l_src):
        own = [
            (0, 1, ymod(yw + 1) * 128, 128, 0),
            (0, 1, ymod(yw + 3) * 128, 128, 128),
            (0, 0, ymod(yw + 2) * 128, 128, 128),
            (0, 3, yw * 128, 128, m128(l_src * 128)),
            (1, 0, lax.div(ymod(yw + 2), 2) * 256, 256, 0),
            (1, 3, lax.div(yw, 2) * 256, 256, 0),
        ]
        hop = [
            (0, 0, ymod(yw + 2) * 128, 128, 0),
            (0, 2, ymod(yw + 1) * 128, 128, 0),
            (0, 2, ymod(yw + 3) * 128, 128, 128),
            (0, 3, yw * 128, 128, m128(l_src * 128)),
            (1, 1, lax.div(ymod(yw + 1), 2) * 256, 128, 0),
            (1, 1, lax.div(ymod(yw + 3), 2) * 256, 128, 128),
            (1, 2, lax.div(ymod(yw + 1), 2) * 256 + 128, 128, 0),
            (1, 2, lax.div(ymod(yw + 3), 2) * 256 + 128, 128, 128),
        ]
        return own, hop

    own, _ = own_parts(y, lo)
    _, hop_out = own_parts(yt, lo)
    _, hop_in = own_parts(y, 1 - lo)
    own_copies = [local(*own_rows(p, j, f, w, t, y), lS.at[i]) for i, (p, j, f, w, t) in enumerate(own)]
    hop_sends = [
        remote(*own_rows(p, j, f, w, t, yt), hS, hR.at[i], pair) for i, (p, j, f, w, t) in enumerate(hop_out)
    ]
    hop_recvs = [
        remote(*own_rows(p, j, f, w, t, y), hS, hR.at[i], pair) for i, (p, j, f, w, t) in enumerate(hop_in)
    ]

    def strip(cc, xx):
        return (cc * 4 + xx) * 256

    def xregion(p, cc, xx, u):
        if p == 0:
            half = lo if u < 2 else 1 - lo
            return A.at[0, pl.ds((u % 2) * 512, 512), pl.ds(m128(strip(cc, xx) + half * 128), 128)]
        return A.at[1, pl.ds(pl.multiple_of(u * 128, 128), 128), pl.ds(m128(strip(cc, xx)), 256)]

    left_copy = local(
        left.at[:, pl.ds(m128(lo * 128), 128)],
        A.at[0, :, pl.ds(m128(strip(c, x) + lo * 128), 128)],
        lS.at[6],
    )
    swaps = [
        remote(
            left.at[pl.ds(u * 512, 512), pl.ds(m128((1 - lo) * 128), 128)],
            A.at[0, pl.ds(u * 512, 512), pl.ds(m128(strip(c, x) + lo * 128), 128)],
            wS, wR.at[u], pair,
        )
        for u in range(2)
    ]
    swap_recvs = [
        remote(
            left.at[pl.ds(u * 512, 512), pl.ds(m128((1 - lo) * 128), 128)],
            A.at[0, pl.ds(u * 512, 512), pl.ds(m128(strip(c, x) + (1 - lo) * 128), 128)],
            wS, wR.at[u], pair,
        )
        for u in range(2)
    ]

    left_copy.start()
    for i in range(6):
        own_copies[i].start()

    for half in range(2):
        B[1, 3, half, zpos(rem(z + 4, 8))] = jnp.zeros((128, 256), BF16)

    pl.semaphore_wait(barrier, 8)

    hop_sends[0].start()
    for u in range(2):
        swaps[u].start()
    for i in range(1, 8):
        hop_sends[i].start()

    OWN_OF = {(0, 0): [2], (0, 1): [0, 1], (0, 2): [], (0, 3): [3], (1, 0): [4], (1, 1): [], (1, 2): [], (1, 3): [5]}
    HOP_OF = {(0, 0): [0], (0, 1): [], (0, 2): [1, 2], (0, 3): [3], (1, 0): [], (1, 1): [4, 5], (1, 2): [6, 7], (1, 3): []}

    def z_copy(s, d, minor, level, part, arriving):
        p, j = STAGES[s]
        sign = -1 if d == 0 else 1
        half = d if minor == 0 else 1 - d
        block = rem(z + sign * (level + (1 if arriving else 0)), 8)
        rows = pl.ds(part * (128 // PARTS[s]), 128 // PARTS[s])
        src = B.at[p, j, half, zpos(block), rows]
        dst = Bx.at[half, rows] if s == LAST and level == 3 else src
        k = FIRST[s] + (d * 7 + level + (4 if minor else 0)) * PARTS[s] + part
        return remote(src, dst, zS.at[p], zR.at[k], z_to[d])

    def z_tick(s, level):
        if level == 0:
            for i in OWN_OF[STAGES[s]]:
                own_copies[i].wait()
            for i in HOP_OF[STAGES[s]]:
                hop_recvs[i].wait_recv()
        for minor in range(1 if level == 3 else 2):
            for part in range(PARTS[s]):
                for d in range(2):
                    if level > 0:
                        z_copy(s, d, minor, level - 1, part, True).wait_recv()
                    z_copy(s, d, minor, level, part, False).start()

    def z_minor(s):
        for part in range(PARTS[s]):
            for d in range(2):
                z_copy(s, d, 1, 2, part, True).wait_recv()

    def z_major(s):
        for part in range(PARTS[s]):
            for d in range(2):
                z_copy(s, d, 0, 3, part, True).wait_recv()

    def z_last(s):
        z_minor(s)
        z_major(s)

    def x_copy(p, d, u, forward, arriving):
        sign = -1 if d == 0 else 1
        away = (1 if forward else 0) + (1 if arriving else 0)
        ref = xregion(p, c, rem(x + sign * away, 4), u)
        k = UNITS[p] + u // 2 if forward else u
        return remote(ref, ref, xS.at[p], xR.at[p * 12 + d * (6, 12)[p] + k], x_to[d])

    def x_forward(p, d, u):
        x_copy(p, d, u, False, True).wait_recv()
        x_copy(p, d, u, True, False).start()

    def d_copy(p, away, g, arriving):
        cc, xx = 1 - c if arriving else c, rem(x + away, 4)
        if p == 0:
            half = lo if g == 0 else 1 - lo
            ref = A.at[0, :, pl.ds(m128(strip(cc, xx) + half * 128), 128)]
        else:
            ref = A.at[1, pl.ds(pl.multiple_of(g * TM, TM), TM), pl.ds(m128(strip(cc, xx)), 256)]
        return remote(ref, ref, dS.at[p], dR.at[p * 8 + away * (2, 4)[p] + g], core)

    def d_all(p, gs):
        for away in range(4):
            for g in gs:
                d_copy(p, away, g, True).wait_recv()

    def x_send_tile(t):
        for u in range(2 * t, 2 * t + 2):
            x_copy(1, 0, u, False, False).start()
            x_copy(1, 1, 4 * t + 1 - u, False, False).start()

    def c_copies(p, j, t, arriving):
        rows = pl.ds(t * TM, TM)
        made = []
        for q in range(2):
            k = 2 * j + q
            if j == 0:
                made.append(
                    remote(
                        send.at[p, 0, rows, pl.ds(q * 128, 128)], relay.at[p, q, rows],
                        cS.at[p], cR.at[p, k, t], y_of[2 * q],
                    )
                )
                continue
            if p == 0:
                which = lo if (j == 1) != arriving else 1 - lo
                place = m128(which * 128)
            else:
                place = (j - 1) * 128
            made.append(
                remote(
                    send.at[p, j, rows, pl.ds(q * 128, 128)],
                    recv.at[p, q, rows, pl.ds(place, 128)],
                    cS.at[p], cR.at[p, k, t], y_of[2 * q],
                )
            )
        return made

    def compute(s, t0, t1):
        p, j = STAGES[s]

        def body(t, carry):
            rows = pl.ds(t * TM if isinstance(t, int) else pl.multiple_of(t * TM, TM), TM)
            acc = jnp.dot(A[p, rows, :], B[p, j].reshape(2048, 256), preferred_element_type=jnp.float32)
            if j in (1, 2):
                q = j - 1
                c_copies(p, 0, t, True)[q].wait_recv()
                halves = [acc[:, :128], acc[:, 128:]]
                halves[q] = halves[q] + relay[p, q, rows, :].astype(jnp.float32)
                acc = jnp.concatenate(halves, axis=1)
            if j < 3:
                send[p, j, rows, :] = acc.astype(BF16)
                for copy in c_copies(p, j, t, False):
                    copy.start()
                return carry
            if s == LAST:
                own_sum[rows, :] = acc
                return carry
            finish(p, t, rows, acc)
            return carry

        if s == LAST:
            for t in range(t0, t1):
                body(t, 0)
            return
        lax.fori_loop(t0, t1, body, 0)

    def finish_last(t0, t1):
        def body(t, carry):
            rows = pl.ds(t * TM if isinstance(t, int) else pl.multiple_of(t * TM, TM), TM)
            far = zpos(rem(z + 4, 8))
            piece = jnp.concatenate(
                [A[1, rows, pl.ds(m128((half * 8 + far) * 128), 128)] for half in range(2)], axis=1
            )
            acc = jnp.dot(piece, Bx[...].reshape(256, 256), preferred_element_type=jnp.float32)
            finish(1, t, rows, own_sum[rows, :] + acc)
            return carry

        lax.fori_loop(t0, t1, body, 0)

    def finish(p, t, rows, acc):
        if True:
            for jj in (1, 2):
                for copy in c_copies(p, jj, t, True):
                    copy.wait_recv()
            for d in range(2):
                acc = acc + recv[p, d, rows, :].astype(jnp.float32)
            if p == 0:
                A[1, rows, pl.ds(m128(strip(c, x)), 256)] = acc.astype(BF16)
                d_copy(1, 0, t, False).start()
            else:
                out[rows, :] = acc.astype(BF16)

    def x_start(u):
        if u == 0:
            left_copy.wait()
        if u >= 2:
            swap_recvs[u - 2].wait_recv()
        for d in range(2):
            x_copy(0, d, u, False, False).start()
        if u % 2 == 1:
            d_copy(0, 0, u // 2, False).start()

    def x_forwards(p, us):
        for u in us:
            x_forward(p, u % 2, u)

    def x_rest(p, g):
        for u in (2 * g, 2 * g + 1):
            x_copy(p, 1 - u % 2, u, False, True).wait_recv()
        for away in (1, 3):
            d_copy(p, away, g, False).start()

    def x_far(p, g):
        for u in (2 * g, 2 * g + 1):
            x_copy(p, u % 2, u, True, True).wait_recv()
        d_copy(p, 2, g, False).start()

    def do(f, *args):
        return lambda: f(*args)

    ACTIONS = {
        0: [do(x_start, 0), do(x_start, 1)],
        1: [do(x_forwards, 0, (0, 1))],
        2: [do(x_start, 2), do(x_rest, 0, 0)],
        3: [do(x_start, 3), do(x_far, 0, 0)],
        4: [do(x_forwards, 0, (2,))],
        5: [do(x_forwards, 0, (3,))],
        7: [do(x_rest, 0, 1)],
        8: [do(x_far, 0, 1)],
        9: [do(d_all, 0, (0, 1))],
        10: [do(z_last, 0), do(compute, 0, 0, 4)],
        11: [do(z_last, 1), do(compute, 1, 0, 2)],
        12: [do(compute, 1, 2, 4)],
        14: [do(z_last, 2), do(compute, 2, 0, 1)],
        16: [do(compute, 2, 1, 4)],
        18: [do(z_last, 3), do(compute, 3, 0, 1), do(x_send_tile, 0), do(compute, 3, 1, 2), do(x_send_tile, 1),
             do(compute, 3, 2, 4)],
        19: [do(x_forwards, 1, (0, 1)), do(x_send_tile, 2)],
        20: [do(x_forwards, 1, (2, 3)), do(x_send_tile, 3), do(x_rest, 1, 0)],
        22: [do(x_rest, 1, 1), do(x_far, 1, 0)],
        23: [do(x_forwards, 1, (4, 5)), do(z_last, 4), do(d_all, 1, (0,)), do(compute, 4, 0, 1), do(x_far, 1, 1)],
        24: [do(x_rest, 1, 2), do(x_forwards, 1, (6, 7)), do(d_all, 1, (1,)), do(compute, 4, 1, 2)],
        25: [do(x_far, 1, 2)],
        26: [do(x_rest, 1, 3)],
        27: [do(d_all, 1, (2,)), do(compute, 4, 2, 3), do(x_far, 1, 3), do(z_last, 5), do(compute, 5, 0, 1), do(d_all, 1, (3,)),
             do(compute, 4, 3, 4), do(compute, 5, 1, 2)],
        28: [do(compute, 5, 2, 4)],
        30: [do(z_last, 6), do(compute, 6, 0, 4)],
        31: [do(z_minor, 7), do(compute, 7, 0, 4), do(z_major, 7), do(finish_last, 0, 4)],
    }
    for i, (s, level) in enumerate(ORDER):
        z_tick(s, level)
        for action in ACTIONS.get(i, ()):
            action()

    def all_sent(ref, sem):
        remote(ref, ref, sem, sem, core).wait_send()

    all_sent(B.at[0, 0, 0], hS)
    all_sent(A.at[0, pl.ds(0, 64)], wS)
    for p in range(2):
        all_sent(B.at[p, :, :, pl.ds(0, 7)], zS.at[p])
        all_sent(A.at[p, pl.ds(0, 384)], xS.at[p])
        all_sent(A.at[p, pl.ds(0, 512)], dS.at[p])
        all_sent(send.at[p], cS.at[p])


def per_device(left, middle, right):
    rows, width = left.shape
    dma = pltpu.SemaphoreType.DMA
    return pl.pallas_call(
        kernel,
        out_shape=jax.ShapeDtypeStruct((rows, width), BF16),
        in_specs=[pl.BlockSpec(memory_space=pl.ANY)] * 3,
        out_specs=pl.BlockSpec(memory_space=pltpu.VMEM),
        scratch_shapes=[
            pltpu.VMEM((2, 1024, 2048), BF16),
            pltpu.VMEM((2, 4, 2, 8, 128, 256), BF16),
            pltpu.VMEM((2, 128, 256), BF16),
            pltpu.VMEM((1024, 256), jnp.float32),
            pltpu.VMEM((2, 3, 1024, 256), BF16),
            pltpu.VMEM((2, 2, 1024, 256), BF16),
            pltpu.VMEM((2, 2, 1024, 128), BF16),
            dma((2,)), dma((FIRST[8],)),
            dma((2,)), dma((36,)),
            dma((2,)), dma((24,)),
            dma((2,)), dma((2, 6, TILES)),
            dma(()), dma((8,)),
            dma(()), dma((2,)),
            dma((7,)),
        ],
        compiler_params=pltpu.CompilerParams(
            collective_id=0, has_side_effects=True, vmem_limit_bytes=int(52 * 1024 * 1024)
        ),
    )(left, middle.reshape(2, rows // 2, -1), right.reshape(2, rows // 2, -1))


def solution(mesh):
    return jax.shard_map(
        per_device,
        mesh=mesh,
        in_specs=(P("row", ("col", "layer")), P("row", "col"), P("row", "col")),
        out_specs=P("row", ("col", "layer")),
        check_vma=False,
    )
```

```python
import jax
import jax.numpy as jnp
from jax import lax
from jax.experimental import pallas as pl
from jax.experimental.pallas import tpu as pltpu
from jax.sharding import PartitionSpec as P

MESH = pl.DeviceIdType.MESH
BF16 = jnp.bfloat16
TM = 256
TILES = 1024 // TM
UNITS = (4, 8)

STAGES = [(0, 0), (0, 1), (0, 2), (0, 3), (1, 0), (1, 1), (1, 2), (1, 3)]

ORDER = [
    (1, 0), (0, 0), (1, 1), (0, 1), (1, 2), (0, 2), (1, 3), (2, 0), (0, 3), (2, 1), (3, 0),
    (2, 2), (3, 1), (2, 3), (3, 2), (4, 0), (3, 3), (4, 1), (5, 0), (4, 2), (5, 1), (4, 3),
    (6, 0), (5, 2), (6, 1), (5, 3), (7, 0), (6, 2), (7, 1), (6, 3), (7, 2), (7, 3),
]
PARTS = (1, 1, 1, 1, 2, 1, 1, 2)
FIRST = [sum(14 * n for n in PARTS[:s]) for s in range(9)]
LAST = 7


def rem(a, n):
    return lax.rem(a + 4 * n, jnp.int32(n))


def kernel(left, middle, right, out, A, B, Bx, own_sum, send, recv, relay,
           zS, zR, xS, xR, dS, dR, cS, cR, hS, hR, wS, wR, lS):
    z = lax.axis_index("row")
    col = lax.axis_index("col")
    h = lax.axis_index("layer")
    c = lax.rem(col, 2)
    x = lax.rem(lax.div(col, 2), 4)
    lo = lax.div(col, 8)
    y = h * 2 + lo

    def dev(zz=None, xx=None, yy=None, cc=None):
        zz = z if zz is None else zz
        xx = x if xx is None else xx
        yy = y if yy is None else yy
        cc = c if cc is None else cc
        return (zz, lax.rem(yy, 2) * 8 + xx * 2 + cc, lax.div(yy, 2))

    z_to = [dev(zz=rem(z + 1, 8)), dev(zz=rem(z - 1, 8))]
    x_to = [dev(xx=rem(x + 1, 4)), dev(xx=rem(x - 1, 4))]
    y_of = [dev(yy=rem(y + d, 4)) for d in (1, 2, 3)]
    pair = dev(yy=h * 2 + 1 - lo)
    yt = h * 2 + 1 - lo
    core = dev(cc=1 - c)

    barrier = pltpu.get_barrier_semaphore()
    for peer in z_to + x_to + y_of + [core]:
        pl.semaphore_signal(barrier, inc=1, device_id=peer, device_id_type=MESH)

    def m128(v):
        return pl.multiple_of(v, 128)

    def zpos(zz):
        return lax.rem(zz, 4) * 2 + lax.div(zz, 4)

    def local(src, dst, sem):
        return pltpu.make_async_copy(src, dst, sem)

    def remote(src, dst, ssem, rsem, to):
        return pltpu.make_async_remote_copy(
            src_ref=src, dst_ref=dst, send_sem=ssem, recv_sem=rsem, device_id=to, device_id_type=MESH
        )

    ymod = lambda v: rem(v, 4)

    def own_rows(p, j, cols_from, width, cols_to, ywho):
        src = (middle, right)[p].at[:, pl.ds(m128(ywho * 128), 128), pl.ds(m128(cols_from), width)]
        dst = B.at[p, j, :, zpos(z), :, pl.ds(cols_to, width)]
        return src, dst

    def own_parts(yw, l_src):
        own = [
            (0, 1, ymod(yw + 1) * 128, 128, 0),
            (0, 1, ymod(yw + 3) * 128, 128, 128),
            (0, 0, ymod(yw + 2) * 128, 128, 128),
            (0, 3, yw * 128, 128, m128(l_src * 128)),
            (1, 0, lax.div(ymod(yw + 2), 2) * 256, 256, 0),
            (1, 3, lax.div(yw, 2) * 256, 256, 0),
        ]
        hop = [
            (0, 0, ymod(yw + 2) * 128, 128, 0),
            (0, 2, ymod(yw + 1) * 128, 128, 0),
            (0, 2, ymod(yw + 3) * 128, 128, 128),
            (0, 3, yw * 128, 128, m128(l_src * 128)),
            (1, 1, lax.div(ymod(yw + 1), 2) * 256, 128, 0),
            (1, 1, lax.div(ymod(yw + 3), 2) * 256, 128, 128),
            (1, 2, lax.div(ymod(yw + 1), 2) * 256 + 128, 128, 0),
            (1, 2, lax.div(ymod(yw + 3), 2) * 256 + 128, 128, 128),
        ]
        return own, hop

    own, _ = own_parts(y, lo)
    _, hop_out = own_parts(yt, lo)
    _, hop_in = own_parts(y, 1 - lo)
    own_copies = [local(*own_rows(p, j, f, w, t, y), lS.at[i]) for i, (p, j, f, w, t) in enumerate(own)]
    hop_sends = [
        remote(*own_rows(p, j, f, w, t, yt), hS, hR.at[i], pair) for i, (p, j, f, w, t) in enumerate(hop_out)
    ]
    hop_recvs = [
        remote(*own_rows(p, j, f, w, t, y), hS, hR.at[i], pair) for i, (p, j, f, w, t) in enumerate(hop_in)
    ]

    def strip(cc, xx):
        return (cc * 4 + xx) * 256

    def xregion(p, cc, xx, u):
        if p == 0:
            half = lo if u < 2 else 1 - lo
            return A.at[0, pl.ds((u % 2) * 512, 512), pl.ds(m128(strip(cc, xx) + half * 128), 128)]
        return A.at[1, pl.ds(pl.multiple_of(u * 128, 128), 128), pl.ds(m128(strip(cc, xx)), 256)]

    left_copy = local(
        left.at[:, pl.ds(m128(lo * 128), 128)],
        A.at[0, :, pl.ds(m128(strip(c, x) + lo * 128), 128)],
        lS.at[6],
    )
    swaps = [
        remote(
            left.at[pl.ds(u * 512, 512), pl.ds(m128((1 - lo) * 128), 128)],
            A.at[0, pl.ds(u * 512, 512), pl.ds(m128(strip(c, x) + lo * 128), 128)],
            wS, wR.at[u], pair,
        )
        for u in range(2)
    ]
    swap_recvs = [
        remote(
            left.at[pl.ds(u * 512, 512), pl.ds(m128((1 - lo) * 128), 128)],
            A.at[0, pl.ds(u * 512, 512), pl.ds(m128(strip(c, x) + (1 - lo) * 128), 128)],
            wS, wR.at[u], pair,
        )
        for u in range(2)
    ]

    left_copy.start()
    for i in range(6):
        own_copies[i].start()

    for half in range(2):
        B[1, 3, half, zpos(rem(z + 4, 8))] = jnp.zeros((128, 256), BF16)

    pl.semaphore_wait(barrier, 8)

    hop_sends[0].start()
    for u in range(2):
        swaps[u].start()
    for i in range(1, 8):
        hop_sends[i].start()

    OWN_OF = {(0, 0): [2], (0, 1): [0, 1], (0, 2): [], (0, 3): [3], (1, 0): [4], (1, 1): [], (1, 2): [], (1, 3): [5]}
    HOP_OF = {(0, 0): [0], (0, 1): [], (0, 2): [1, 2], (0, 3): [3], (1, 0): [], (1, 1): [4, 5], (1, 2): [6, 7], (1, 3): []}

    def z_copy(s, d, minor, level, part, arriving):
        p, j = STAGES[s]
        sign = -1 if d == 0 else 1
        half = d if minor == 0 else 1 - d
        block = rem(z + sign * (level + (1 if arriving else 0)), 8)
        rows = pl.ds(part * (128 // PARTS[s]), 128 // PARTS[s])
        src = B.at[p, j, half, zpos(block), rows]
        dst = Bx.at[half, rows] if s == LAST and level == 3 else src
        k = FIRST[s] + (d * 7 + level + (4 if minor else 0)) * PARTS[s] + part
        return remote(src, dst, zS.at[p], zR.at[k], z_to[d])

    def z_tick(s, level):
        if level == 0:
            for i in OWN_OF[STAGES[s]]:
                own_copies[i].wait()
            for i in HOP_OF[STAGES[s]]:
                hop_recvs[i].wait_recv()
        for minor in range(1 if level == 3 else 2):
            for part in range(PARTS[s]):
                for d in range(2):
                    if level > 0:
                        z_copy(s, d, minor, level - 1, part, True).wait_recv()
                    z_copy(s, d, minor, level, part, False).start()

    def z_minor(s):
        for part in range(PARTS[s]):
            for d in range(2):
                z_copy(s, d, 1, 2, part, True).wait_recv()

    def z_major(s):
        for part in range(PARTS[s]):
            for d in range(2):
                z_copy(s, d, 0, 3, part, True).wait_recv()

    def z_last(s):
        z_minor(s)
        z_major(s)

    def x_copy(p, d, u, forward, arriving):
        sign = -1 if d == 0 else 1
        away = (1 if forward else 0) + (1 if arriving else 0)
        ref = xregion(p, c, rem(x + sign * away, 4), u)
        k = UNITS[p] + u // 2 if forward else u
        return remote(ref, ref, xS.at[p], xR.at[p * 12 + d * (6, 12)[p] + k], x_to[d])

    def x_forward(p, d, u):
        x_copy(p, d, u, False, True).wait_recv()
        x_copy(p, d, u, True, False).start()

    def d_copy(p, away, g, arriving):
        cc, xx = 1 - c if arriving else c, rem(x + away, 4)
        if p == 0:
            half = lo if g == 0 else 1 - lo
            ref = A.at[0, :, pl.ds(m128(strip(cc, xx) + half * 128), 128)]
        else:
            ref = A.at[1, pl.ds(pl.multiple_of(g * TM, TM), TM), pl.ds(m128(strip(cc, xx)), 256)]
        return remote(ref, ref, dS.at[p], dR.at[p * 8 + away * (2, 4)[p] + g], core)

    def d_all(p, gs):
        for away in range(4):
            for g in gs:
                d_copy(p, away, g, True).wait_recv()

    def x_send_tile(t):
        for u in range(2 * t, 2 * t + 2):
            x_copy(1, 0, u, False, False).start()
            x_copy(1, 1, 4 * t + 1 - u, False, False).start()

    def c_copies(p, j, t, arriving):
        rows = pl.ds(t * TM, TM)
        made = []
        for q in range(2):
            k = 2 * j + q
            if j == 0:
                made.append(
                    remote(
                        send.at[p, 0, rows, pl.ds(q * 128, 128)], relay.at[p, q, rows],
                        cS.at[p], cR.at[p, k, t], y_of[2 * q],
                    )
                )
                continue
            if p == 0:
                which = lo if (j == 1) != arriving else 1 - lo
                place = m128(which * 128)
            else:
                place = (j - 1) * 128
            made.append(
                remote(
                    send.at[p, j, rows, pl.ds(q * 128, 128)],
                    recv.at[p, q, rows, pl.ds(place, 128)],
                    cS.at[p], cR.at[p, k, t], y_of[2 * q],
                )
            )
        return made

    def compute(s, t0, t1):
        p, j = STAGES[s]

        def body(t, carry):
            rows = pl.ds(t * TM if isinstance(t, int) else pl.multiple_of(t * TM, TM), TM)
            acc = jnp.dot(A[p, rows, :], B[p, j].reshape(2048, 256), preferred_element_type=jnp.float32)
            if j in (1, 2):
                q = j - 1
                c_copies(p, 0, t, True)[q].wait_recv()
                halves = [acc[:, :128], acc[:, 128:]]
                halves[q] = halves[q] + relay[p, q, rows, :].astype(jnp.float32)
                acc = jnp.concatenate(halves, axis=1)
            if j < 3:
                send[p, j, rows, :] = acc.astype(BF16)
                for copy in c_copies(p, j, t, False):
                    copy.start()
                return carry
            if s == LAST:
                own_sum[rows, :] = acc
                return carry
            finish(p, t, rows, acc)
            return carry

        if s == LAST:
            for t in range(t0, t1):
                body(t, 0)
            return
        lax.fori_loop(t0, t1, body, 0)

    def finish_last(t0, t1):
        def body(t, carry):
            rows = pl.ds(t * TM if isinstance(t, int) else pl.multiple_of(t * TM, TM), TM)
            far = zpos(rem(z + 4, 8))
            piece = jnp.concatenate(
                [A[1, rows, pl.ds(m128((half * 8 + far) * 128), 128)] for half in range(2)], axis=1
            )
            acc = jnp.dot(piece, Bx[...].reshape(256, 256), preferred_element_type=jnp.float32)
            finish(1, t, rows, own_sum[rows, :] + acc)
            return carry

        lax.fori_loop(t0, t1, body, 0)

    def finish(p, t, rows, acc):
        if True:
            for jj in (1, 2):
                for copy in c_copies(p, jj, t, True):
                    copy.wait_recv()
            for d in range(2):
                acc = acc + recv[p, d, rows, :].astype(jnp.float32)
            if p == 0:
                A[1, rows, pl.ds(m128(strip(c, x)), 256)] = acc.astype(BF16)
                d_copy(1, 0, t, False).start()
            else:
                out[rows, :] = acc.astype(BF16)

    def x_start(u):
        if u == 0:
            left_copy.wait()
        if u >= 2:
            swap_recvs[u - 2].wait_recv()
        for d in range(2):
            x_copy(0, d, u, False, False).start()
        if u % 2 == 1:
            d_copy(0, 0, u // 2, False).start()

    def x_forwards(p, us):
        for u in us:
            x_forward(p, u % 2, u)

    def x_rest(p, g):
        for u in (2 * g, 2 * g + 1):
            x_copy(p, 1 - u % 2, u, False, True).wait_recv()
        for away in (1, 3):
            d_copy(p, away, g, False).start()

    def x_far(p, g):
        for u in (2 * g, 2 * g + 1):
            x_copy(p, u % 2, u, True, True).wait_recv()
        d_copy(p, 2, g, False).start()

    def do(f, *args):
        return lambda: f(*args)

    ACTIONS = {
        0: [do(x_start, 0), do(x_start, 1)],
        1: [do(x_forwards, 0, (0, 1))],
        2: [do(x_start, 2), do(x_rest, 0, 0)],
        3: [do(x_start, 3), do(x_far, 0, 0)],
        4: [do(x_forwards, 0, (2,))],
        5: [do(x_forwards, 0, (3,))],
        7: [do(x_rest, 0, 1)],
        8: [do(x_far, 0, 1)],
        9: [do(d_all, 0, (0, 1))],
        10: [do(z_last, 0), do(compute, 0, 0, 4)],
        11: [do(z_last, 1), do(compute, 1, 0, 2)],
        12: [do(compute, 1, 2, 4)],
        14: [do(z_last, 2), do(compute, 2, 0, 1)],
        16: [do(compute, 2, 1, 4)],
        18: [do(z_last, 3), do(compute, 3, 0, 1), do(x_send_tile, 0), do(compute, 3, 1, 2), do(x_send_tile, 1),
             do(compute, 3, 2, 4)],
        19: [do(x_forwards, 1, (0, 1)), do(x_send_tile, 2)],
        20: [do(x_forwards, 1, (2, 3)), do(x_send_tile, 3), do(x_rest, 1, 0)],
        22: [do(x_rest, 1, 1), do(x_far, 1, 0)],
        23: [do(x_forwards, 1, (4, 5)), do(z_last, 4), do(d_all, 1, (0,)), do(compute, 4, 0, 1), do(x_far, 1, 1)],
        24: [do(x_rest, 1, 2), do(x_forwards, 1, (6, 7)), do(d_all, 1, (1,)), do(compute, 4, 1, 2)],
        25: [do(x_far, 1, 2)],
        26: [do(x_rest, 1, 3)],
        27: [do(d_all, 1, (2,)), do(compute, 4, 2, 3), do(x_far, 1, 3), do(z_last, 5), do(compute, 5, 0, 1), do(d_all, 1, (3,)),
             do(compute, 4, 3, 4), do(compute, 5, 1, 2)],
        28: [do(compute, 5, 2, 4)],
        30: [do(z_last, 6), do(compute, 6, 0, 4)],
        31: [do(z_minor, 7), do(compute, 7, 0, 4), do(z_major, 7), do(finish_last, 0, 4)],
    }
    for i, (s, level) in enumerate(ORDER):
        z_tick(s, level)
        for action in ACTIONS.get(i, ()):
            action()

    def all_sent(ref, sem):
        remote(ref, ref, sem, sem, core).wait_send()

    all_sent(B.at[0, 0, 0], hS)
    all_sent(A.at[0, pl.ds(0, 64)], wS)
    for p in range(2):
        all_sent(B.at[p, :, :, pl.ds(0, 7)], zS.at[p])
        all_sent(A.at[p, pl.ds(0, 384)], xS.at[p])
        all_sent(A.at[p, pl.ds(0, 512)], dS.at[p])
        all_sent(send.at[p], cS.at[p])


def per_device(left, middle, right):
    rows, width = left.shape
    dma = pltpu.SemaphoreType.DMA
    return pl.pallas_call(
        kernel,
        out_shape=jax.ShapeDtypeStruct((rows, width), BF16),
        in_specs=[pl.BlockSpec(memory_space=pl.ANY)] * 3,
        out_specs=pl.BlockSpec(memory_space=pltpu.VMEM),
        scratch_shapes=[
            pltpu.VMEM((2, 1024, 2048), BF16),
            pltpu.VMEM((2, 4, 2, 8, 128, 256), BF16),
            pltpu.VMEM((2, 128, 256), BF16),
            pltpu.VMEM((1024, 256), jnp.float32),
            pltpu.VMEM((2, 3, 1024, 256), BF16),
            pltpu.VMEM((2, 2, 1024, 256), BF16),
            pltpu.VMEM((2, 2, 1024, 128), BF16),
            dma((2,)), dma((FIRST[8],)),
            dma((2,)), dma((36,)),
            dma((2,)), dma((24,)),
            dma((2,)), dma((2, 6, TILES)),
            dma(()), dma((8,)),
            dma(()), dma((2,)),
            dma((7,)),
        ],
        compiler_params=pltpu.CompilerParams(
            collective_id=0, has_side_effects=True, vmem_limit_bytes=int(52 * 1024 * 1024)
        ),
    )(left, middle.reshape(2, rows // 2, -1), right.reshape(2, rows // 2, -1))


def solution(mesh):
    return jax.shard_map(
        per_device,
        mesh=mesh,
        in_specs=(P("row", ("col", "layer")), P("row", "col"), P("row", "col")),
        out_specs=P("row", ("col", "layer")),
        check_vma=False,
    )
```

```python
import jax
import jax.numpy as jnp
from jax import lax
from jax.experimental import pallas as pl
from jax.experimental.pallas import tpu as pltpu
from jax.sharding import PartitionSpec as P

MESH = pl.DeviceIdType.MESH
BF16 = jnp.bfloat16
TM = 256
TILES = 1024 // TM
UNITS = (4, 8)

STAGES = [(0, 0), (0, 1), (0, 2), (0, 3), (1, 0), (1, 1), (1, 2), (1, 3)]

ORDER = [
    (1, 0), (0, 0), (1, 1), (0, 1), (1, 2), (0, 2), (1, 3), (2, 0), (0, 3), (2, 1), (3, 0),
    (2, 2), (3, 1), (2, 3), (3, 2), (4, 0), (3, 3), (4, 1), (5, 0), (4, 2), (5, 1), (4, 3),
    (6, 0), (5, 2), (6, 1), (5, 3), (7, 0), (6, 2), (7, 1), (6, 3), (7, 2), (7, 3),
]
PARTS = (1, 1, 1, 1, 2, 1, 1, 2)
FIRST = [sum(14 * n for n in PARTS[:s]) for s in range(9)]
LAST = 7


def rem(a, n):
    return lax.rem(a + 4 * n, jnp.int32(n))


def kernel(left, middle, right, out, A, B, Bx, own_sum, send, recv, relay,
           zS, zR, xS, xR, dS, dR, cS, cR, hS, hR, wS, wR, lS):
    z = lax.axis_index("row")
    col = lax.axis_index("col")
    h = lax.axis_index("layer")
    c = lax.rem(col, 2)
    x = lax.rem(lax.div(col, 2), 4)
    lo = lax.div(col, 8)
    y = h * 2 + lo

    def dev(zz=None, xx=None, yy=None, cc=None):
        zz = z if zz is None else zz
        xx = x if xx is None else xx
        yy = y if yy is None else yy
        cc = c if cc is None else cc
        return (zz, lax.rem(yy, 2) * 8 + xx * 2 + cc, lax.div(yy, 2))

    z_to = [dev(zz=rem(z + 1, 8)), dev(zz=rem(z - 1, 8))]
    x_to = [dev(xx=rem(x + 1, 4)), dev(xx=rem(x - 1, 4))]
    y_of = [dev(yy=rem(y + d, 4)) for d in (1, 2, 3)]
    pair = dev(yy=h * 2 + 1 - lo)
    yt = h * 2 + 1 - lo
    core = dev(cc=1 - c)

    barrier = pltpu.get_barrier_semaphore()
    for peer in z_to + x_to + y_of + [core]:
        pl.semaphore_signal(barrier, inc=1, device_id=peer, device_id_type=MESH)

    def m128(v):
        return pl.multiple_of(v, 128)

    def zpos(zz):
        return lax.rem(zz, 4) * 2 + lax.div(zz, 4)

    def local(src, dst, sem):
        return pltpu.make_async_copy(src, dst, sem)

    def remote(src, dst, ssem, rsem, to):
        return pltpu.make_async_remote_copy(
            src_ref=src, dst_ref=dst, send_sem=ssem, recv_sem=rsem, device_id=to, device_id_type=MESH
        )

    ymod = lambda v: rem(v, 4)

    def own_rows(p, j, cols_from, width, cols_to, ywho):
        src = (middle, right)[p].at[:, pl.ds(m128(ywho * 128), 128), pl.ds(m128(cols_from), width)]
        dst = B.at[p, j, :, zpos(z), :, pl.ds(cols_to, width)]
        return src, dst

    def own_parts(yw, l_src):
        own = [
            (0, 1, ymod(yw + 1) * 128, 128, 0),
            (0, 1, ymod(yw + 3) * 128, 128, 128),
            (0, 0, ymod(yw + 2) * 128, 128, 128),
            (0, 3, yw * 128, 128, m128(l_src * 128)),
            (1, 0, lax.div(ymod(yw + 2), 2) * 256, 256, 0),
            (1, 3, lax.div(yw, 2) * 256, 256, 0),
        ]
        hop = [
            (0, 0, ymod(yw + 2) * 128, 128, 0),
            (0, 2, ymod(yw + 1) * 128, 128, 0),
            (0, 2, ymod(yw + 3) * 128, 128, 128),
            (0, 3, yw * 128, 128, m128(l_src * 128)),
            (1, 1, lax.div(ymod(yw + 1), 2) * 256, 128, 0),
            (1, 1, lax.div(ymod(yw + 3), 2) * 256, 128, 128),
            (1, 2, lax.div(ymod(yw + 1), 2) * 256 + 128, 128, 0),
            (1, 2, lax.div(ymod(yw + 3), 2) * 256 + 128, 128, 128),
        ]
        return own, hop

    own, _ = own_parts(y, lo)
    _, hop_out = own_parts(yt, lo)
    _, hop_in = own_parts(y, 1 - lo)
    own_copies = [local(*own_rows(p, j, f, w, t, y), lS.at[i]) for i, (p, j, f, w, t) in enumerate(own)]
    hop_sends = [
        remote(*own_rows(p, j, f, w, t, yt), hS, hR.at[i], pair) for i, (p, j, f, w, t) in enumerate(hop_out)
    ]
    hop_recvs = [
        remote(*own_rows(p, j, f, w, t, y), hS, hR.at[i], pair) for i, (p, j, f, w, t) in enumerate(hop_in)
    ]

    def strip(cc, xx):
        return (cc * 4 + xx) * 256

    def xregion(p, cc, xx, u):
        if p == 0:
            half = lo if u < 2 else 1 - lo
            return A.at[0, pl.ds((u % 2) * 512, 512), pl.ds(m128(strip(cc, xx) + half * 128), 128)]
        return A.at[1, pl.ds(pl.multiple_of(u * 128, 128), 128), pl.ds(m128(strip(cc, xx)), 256)]

    left_copy = local(
        left.at[:, pl.ds(m128(lo * 128), 128)],
        A.at[0, :, pl.ds(m128(strip(c, x) + lo * 128), 128)],
        lS.at[6],
    )
    swaps = [
        remote(
            left.at[pl.ds(u * 512, 512), pl.ds(m128((1 - lo) * 128), 128)],
            A.at[0, pl.ds(u * 512, 512), pl.ds(m128(strip(c, x) + lo * 128), 128)],
            wS, wR.at[u], pair,
        )
        for u in range(2)
    ]
    swap_recvs = [
        remote(
            left.at[pl.ds(u * 512, 512), pl.ds(m128((1 - lo) * 128), 128)],
            A.at[0, pl.ds(u * 512, 512), pl.ds(m128(strip(c, x) + (1 - lo) * 128), 128)],
            wS, wR.at[u], pair,
        )
        for u in range(2)
    ]

    left_copy.start()
    for i in range(6):
        own_copies[i].start()

    for half in range(2):
        B[1, 3, half, zpos(rem(z + 4, 8))] = jnp.zeros((128, 256), BF16)

    pl.semaphore_wait(barrier, 8)

    hop_sends[0].start()
    for u in range(2):
        swaps[u].start()
    for i in range(1, 8):
        hop_sends[i].start()

    OWN_OF = {(0, 0): [2], (0, 1): [0, 1], (0, 2): [], (0, 3): [3], (1, 0): [4], (1, 1): [], (1, 2): [], (1, 3): [5]}
    HOP_OF = {(0, 0): [0], (0, 1): [], (0, 2): [1, 2], (0, 3): [3], (1, 0): [], (1, 1): [4, 5], (1, 2): [6, 7], (1, 3): []}

    def z_copy(s, d, minor, level, part, arriving):
        p, j = STAGES[s]
        sign = -1 if d == 0 else 1
        half = d if minor == 0 else 1 - d
        block = rem(z + sign * (level + (1 if arriving else 0)), 8)
        rows = pl.ds(part * (128 // PARTS[s]), 128 // PARTS[s])
        src = B.at[p, j, half, zpos(block), rows]
        dst = Bx.at[half, rows] if s == LAST and level == 3 else src
        k = FIRST[s] + (d * 7 + level + (4 if minor else 0)) * PARTS[s] + part
        return remote(src, dst, zS.at[p], zR.at[k], z_to[d])

    def z_tick(s, level):
        if level == 0:
            for i in OWN_OF[STAGES[s]]:
                own_copies[i].wait()
            for i in HOP_OF[STAGES[s]]:
                hop_recvs[i].wait_recv()
        for minor in range(1 if level == 3 else 2):
            for part in range(PARTS[s]):
                for d in range(2):
                    if level > 0:
                        z_copy(s, d, minor, level - 1, part, True).wait_recv()
                    z_copy(s, d, minor, level, part, False).start()

    def z_minor(s):
        for part in range(PARTS[s]):
            for d in range(2):
                z_copy(s, d, 1, 2, part, True).wait_recv()

    def z_major(s):
        for part in range(PARTS[s]):
            for d in range(2):
                z_copy(s, d, 0, 3, part, True).wait_recv()

    def z_last(s):
        z_minor(s)
        z_major(s)

    def x_copy(p, d, u, forward, arriving):
        sign = -1 if d == 0 else 1
        away = (1 if forward else 0) + (1 if arriving else 0)
        ref = xregion(p, c, rem(x + sign * away, 4), u)
        k = UNITS[p] + u // 2 if forward else u
        return remote(ref, ref, xS.at[p], xR.at[p * 12 + d * (6, 12)[p] + k], x_to[d])

    def x_forward(p, d, u):
        x_copy(p, d, u, False, True).wait_recv()
        x_copy(p, d, u, True, False).start()

    def d_copy(p, away, g, arriving):
        cc, xx = 1 - c if arriving else c, rem(x + away, 4)
        if p == 0:
            half = lo if g == 0 else 1 - lo
            ref = A.at[0, :, pl.ds(m128(strip(cc, xx) + half * 128), 128)]
        else:
            ref = A.at[1, pl.ds(pl.multiple_of(g * TM, TM), TM), pl.ds(m128(strip(cc, xx)), 256)]
        return remote(ref, ref, dS.at[p], dR.at[p * 8 + away * (2, 4)[p] + g], core)

    def d_all(p, gs):
        for away in range(4):
            for g in gs:
                d_copy(p, away, g, True).wait_recv()

    def x_send_tile(t):
        for u in range(2 * t, 2 * t + 2):
            x_copy(1, 0, u, False, False).start()
            x_copy(1, 1, 4 * t + 1 - u, False, False).start()

    def c_copies(p, j, t, arriving):
        rows = pl.ds(t * TM, TM)
        made = []
        for q in range(2):
            k = 2 * j + q
            if j == 0:
                made.append(
                    remote(
                        send.at[p, 0, rows, pl.ds(q * 128, 128)], relay.at[p, q, rows],
                        cS.at[p], cR.at[p, k, t], y_of[2 * q],
                    )
                )
                continue
            if p == 0:
                which = lo if (j == 1) != arriving else 1 - lo
                place = m128(which * 128)
            else:
                place = (j - 1) * 128
            made.append(
                remote(
                    send.at[p, j, rows, pl.ds(q * 128, 128)],
                    recv.at[p, q, rows, pl.ds(place, 128)],
                    cS.at[p], cR.at[p, k, t], y_of[2 * q],
                )
            )
        return made

    def compute(s, t0, t1):
        p, j = STAGES[s]

        def body(t, carry):
            rows = pl.ds(t * TM if isinstance(t, int) else pl.multiple_of(t * TM, TM), TM)
            acc = jnp.dot(A[p, rows, :], B[p, j].reshape(2048, 256), preferred_element_type=jnp.float32)
            if j in (1, 2):
                q = j - 1
                c_copies(p, 0, t, True)[q].wait_recv()
                halves = [acc[:, :128], acc[:, 128:]]
                halves[q] = halves[q] + relay[p, q, rows, :].astype(jnp.float32)
                acc = jnp.concatenate(halves, axis=1)
            if j < 3:
                send[p, j, rows, :] = acc.astype(BF16)
                for copy in c_copies(p, j, t, False):
                    copy.start()
                return carry
            if s == LAST:
                own_sum[rows, :] = acc
                return carry
            finish(p, t, rows, acc)
            return carry

        if s == LAST:
            for t in range(t0, t1):
                body(t, 0)
            return
        lax.fori_loop(t0, t1, body, 0)

    def finish_last(t0, t1):
        def body(t, carry):
            rows = pl.ds(t * TM if isinstance(t, int) else pl.multiple_of(t * TM, TM), TM)
            far = zpos(rem(z + 4, 8))
            piece = jnp.concatenate(
                [A[1, rows, pl.ds(m128((half * 8 + far) * 128), 128)] for half in range(2)], axis=1
            )
            acc = jnp.dot(piece, Bx[...].reshape(256, 256), preferred_element_type=jnp.float32)
            finish(1, t, rows, own_sum[rows, :] + acc)
            return carry

        lax.fori_loop(t0, t1, body, 0)

    def finish(p, t, rows, acc):
        if True:
            for jj in (1, 2):
                for copy in c_copies(p, jj, t, True):
                    copy.wait_recv()
            for d in range(2):
                acc = acc + recv[p, d, rows, :].astype(jnp.float32)
            if p == 0:
                A[1, rows, pl.ds(m128(strip(c, x)), 256)] = acc.astype(BF16)
                d_copy(1, 0, t, False).start()
            else:
                out[rows, :] = acc.astype(BF16)

    def x_start(u):
        if u == 0:
            left_copy.wait()
        if u >= 2:
            swap_recvs[u - 2].wait_recv()
        for d in range(2):
            x_copy(0, d, u, False, False).start()
        if u % 2 == 1:
            d_copy(0, 0, u // 2, False).start()

    def x_forwards(p, us):
        for u in us:
            x_forward(p, u % 2, u)

    def x_rest(p, g):
        for u in (2 * g, 2 * g + 1):
            x_copy(p, 1 - u % 2, u, False, True).wait_recv()
        for away in (1, 3):
            d_copy(p, away, g, False).start()

    def x_far(p, g):
        for u in (2 * g, 2 * g + 1):
            x_copy(p, u % 2, u, True, True).wait_recv()
        d_copy(p, 2, g, False).start()

    def do(f, *args):
        return lambda: f(*args)

    ACTIONS = {
        0: [do(x_start, 0), do(x_start, 1)],
        1: [do(x_forwards, 0, (0, 1))],
        2: [do(x_start, 2), do(x_rest, 0, 0)],
        3: [do(x_start, 3), do(x_far, 0, 0)],
        4: [do(x_forwards, 0, (2,))],
        5: [do(x_forwards, 0, (3,))],
        7: [do(x_rest, 0, 1)],
        8: [do(x_far, 0, 1)],
        9: [do(d_all, 0, (0, 1))],
        10: [do(z_last, 0), do(compute, 0, 0, 4)],
        11: [do(z_last, 1), do(compute, 1, 0, 2)],
        12: [do(compute, 1, 2, 4)],
        14: [do(z_last, 2), do(compute, 2, 0, 1)],
        16: [do(compute, 2, 1, 4)],
        18: [do(z_last, 3), do(compute, 3, 0, 1), do(x_send_tile, 0), do(compute, 3, 1, 2), do(x_send_tile, 1),
             do(compute, 3, 2, 4)],
        19: [do(x_forwards, 1, (0, 1)), do(x_send_tile, 2)],
        20: [do(x_forwards, 1, (2, 3)), do(x_send_tile, 3), do(x_rest, 1, 0)],
        22: [do(x_rest, 1, 1), do(x_far, 1, 0)],
        23: [do(x_forwards, 1, (4, 5)), do(z_last, 4), do(d_all, 1, (0,)), do(compute, 4, 0, 1), do(x_far, 1, 1)],
        24: [do(x_rest, 1, 2), do(x_forwards, 1, (6, 7)), do(d_all, 1, (1,)), do(compute, 4, 1, 2)],
        25: [do(x_far, 1, 2)],
        26: [do(x_rest, 1, 3)],
        27: [do(d_all, 1, (2,)), do(compute, 4, 2, 3), do(x_far, 1, 3), do(z_last, 5), do(compute, 5, 0, 1), do(d_all, 1, (3,)),
             do(compute, 4, 3, 4), do(compute, 5, 1, 2)],
        28: [do(compute, 5, 2, 4)],
        30: [do(z_last, 6), do(compute, 6, 0, 2)],
        31: [do(compute, 6, 2, 4), do(z_minor, 7), do(compute, 7, 0, 4), do(z_major, 7), do(finish_last, 0, 4)],
    }
    for i, (s, level) in enumerate(ORDER):
        z_tick(s, level)
        for action in ACTIONS.get(i, ()):
            action()

    def all_sent(ref, sem):
        remote(ref, ref, sem, sem, core).wait_send()

    all_sent(B.at[0, 0, 0], hS)
    all_sent(A.at[0, pl.ds(0, 64)], wS)
    for p in range(2):
        all_sent(B.at[p, :, :, pl.ds(0, 7)], zS.at[p])
        all_sent(A.at[p, pl.ds(0, 384)], xS.at[p])
        all_sent(A.at[p, pl.ds(0, 512)], dS.at[p])
        all_sent(send.at[p], cS.at[p])


def per_device(left, middle, right):
    rows, width = left.shape
    dma = pltpu.SemaphoreType.DMA
    return pl.pallas_call(
        kernel,
        out_shape=jax.ShapeDtypeStruct((rows, width), BF16),
        in_specs=[pl.BlockSpec(memory_space=pl.ANY)] * 3,
        out_specs=pl.BlockSpec(memory_space=pltpu.VMEM),
        scratch_shapes=[
            pltpu.VMEM((2, 1024, 2048), BF16),
            pltpu.VMEM((2, 4, 2, 8, 128, 256), BF16),
            pltpu.VMEM((2, 128, 256), BF16),
            pltpu.VMEM((1024, 256), jnp.float32),
            pltpu.VMEM((2, 3, 1024, 256), BF16),
            pltpu.VMEM((2, 2, 1024, 256), BF16),
            pltpu.VMEM((2, 2, 1024, 128), BF16),
            dma((2,)), dma((FIRST[8],)),
            dma((2,)), dma((36,)),
            dma((2,)), dma((24,)),
            dma((2,)), dma((2, 6, TILES)),
            dma(()), dma((8,)),
            dma(()), dma((2,)),
            dma((7,)),
        ],
        compiler_params=pltpu.CompilerParams(
            collective_id=0, has_side_effects=True, vmem_limit_bytes=int(52 * 1024 * 1024)
        ),
    )(left, middle.reshape(2, rows // 2, -1), right.reshape(2, rows // 2, -1))


def solution(mesh):
    return jax.shard_map(
        per_device,
        mesh=mesh,
        in_specs=(P("row", ("col", "layer")), P("row", "col"), P("row", "col")),
        out_specs=P("row", ("col", "layer")),
        check_vma=False,
    )
```
